8 devices in a mesh: data: 2 (over z, y), tp: 4 (over x, core).
Axes of the slice: x: 2, y: 2, z: 1, core: 2. Of those that a mesh axis runs over, the one named last changes fastest.
Arguments:
- x: bfloat16 [2048, 49152], P('data', 'tp'), parts along dimension 0
- w: bfloat16 [49152, 12288], P('tp')
- lengths: int32 [8], P('data'), parts along dimension 0
Outputs:
- output: bfloat16 [2048, 12288], P('data'), parts along dimension 0
There are 2 independent parts. The reference program is written for one: setup_inputs(seed, part) draws one part's arguments, and reference() takes and returns one part's arrays. A program takes and returns all parts, laid end to end along the dimension named above; an argument that names none is the same for every part.
All inputs are finite; a program needn't handle non-finite values.
Results may differ from the reference program's by a relative error of at most 0.001.
Values are sent between devices in bfloat16 or wider.
A program may use at most 1.5 GiB of HBM per device.

```python
import jax
import jax.numpy as jnp

D = 12288
FF = 49152
TOKENS = 1024
SEQS = 4
SEQ_LEN = TOKENS // SEQS


def draw_lengths(key_len):
    key_draw, key_perm = jax.random.split(key_len)
    lengths = jax.random.randint(key_draw, (SEQS,), 1, SEQ_LEN + 1, dtype=jnp.int32)
    slot_order = jax.random.permutation(key_perm, SEQS)
    lengths = lengths.at[slot_order[0]].set(SEQ_LEN)
    lengths = lengths.at[slot_order[1]].set(1)
    return lengths


def setup_inputs(seed: int = 0, part: int = 0) -> dict:
    key = jax.random.key(seed)
    key_x, key_w, key_len = jax.random.split(key, 3)
    tok_acts = jax.random.normal(jax.random.fold_in(key_x, part), (TOKENS, FF), jnp.float32)
    weight = jax.random.normal(key_w, (FF, D), jnp.float32) * (FF ** -0.5)
    lengths = draw_lengths(jax.random.fold_in(key_len, part))
    return {"x": tok_acts.astype(jnp.bfloat16), "w": weight.astype(jnp.bfloat16), "lengths": lengths}


def reference(x, w, lengths):
    seq_len = x.shape[0] // lengths.shape[0]
    valid = (jnp.arange(seq_len, dtype=jnp.int32)[None, :] < lengths[:, None]).reshape(-1)
    full_sum = jnp.dot(x, w, preferred_element_type=jnp.float32)
    return jnp.where(valid[:, None], full_sum, 0.0).astype(jnp.bfloat16)
```

```python
import functools

import jax
import jax.numpy as jnp
from jax import lax
from jax.experimental import pallas as pl
from jax.experimental.pallas import tpu as pltpu
from jax.sharding import PartitionSpec as P

MESH = pl.DeviceIdType.MESH
TILE = 16
NB = 256
HB = NB // 2
XC = 2048
KC = 6144
BUCKETS = (320, 384, 448, 512, 576, 640, 704, 784)
LAST = 7


def tile_offsets(lens_ref, slots):
    offs, total = [], 0
    for s in range(slots):
        offs.append(total)
        total = total + (lens_ref[s] + TILE - 1) // TILE
    return offs, total


def fused_kernel(rows, table_ref, x_ref, w_ref, y_ref, xp, stage0, stage1, wbuf, part, ra, sb, so, rb, out,
                 xsem, wsem, send_a, recv_a, send_b, recv_b, send_c, recv_c, send_e, recv_e, send_d, recv_d, osem):
    depth, cols = w_ref.shape
    blocks = cols // NB
    half = rows // 2
    stages = (stage0, stage1)
    me = lax.axis_index("tp")
    core = lax.rem(me, 2)
    chip = me // 2
    sibling = {"tp": me + 1 - 2 * core}
    peer = {"tp": lax.rem(me + 2, 4)}
    nx = depth // XC
    nk = depth // KC

    def x_copy(k):
        return pltpu.make_async_copy(x_ref.at[:, :, pl.ds(k * XC, XC)], stages[k % 2], xsem.at[k % 2])

    def w_copy(b):
        s = lax.rem(b, 2)
        return pltpu.make_async_copy(w_ref.at[:, pl.ds(pl.multiple_of(b * NB, NB), NB)], wbuf.at[s], wsem.at[s])

    def remote(src, dst, ssem, rsem, to):
        return pltpu.make_async_remote_copy(src_ref=src, dst_ref=dst, send_sem=ssem, recv_sem=rsem, device_id=to, device_id_type=MESH)

    def copy_a(b):
        s = lax.rem(b, 2)
        return remote(part.at[s, 1 - core], ra.at[s], send_a.at[s], recv_a.at[s], sibling)

    def copy_b(b):
        s, r = lax.rem(b, 4), lax.rem(b, 8)
        return remote(sb.at[s], rb.at[r], send_b.at[s], recv_b.at[r], peer)

    def copy_c(b):
        r = lax.rem(b, 8)
        return remote(out.at[r, core, chip], out.at[r, core, chip], send_c.at[r], recv_c.at[r], peer)

    def copy_e(b):
        r = lax.rem(b, 8)
        return remote(out.at[r, core, chip], out.at[r, core, chip], send_e.at[r], recv_e.at[r], sibling)

    def copy_d(b):
        r = lax.rem(b, 8)
        return remote(out.at[r, core, 1 - chip], out.at[r, core, 1 - chip], send_d.at[r], recv_d.at[r], sibling)

    def copy_o(b):
        r = lax.rem(b, 8)
        return pltpu.make_async_copy(out.at[r], y_ref.at[b], osem.at[r])

    x_copy(0).start()
    w_copy(0).start()

    barrier = pltpu.get_barrier_semaphore()
    for other in (sibling, peer):
        pl.semaphore_signal(barrier, inc=1, device_id=other, device_id_type=MESH)
    pl.semaphore_wait(barrier, 2)

    for k in range(nx):
        if k + 1 < nx:
            x_copy(k + 1).start()
        x_copy(k).wait()

        def tile(t, carry, k=k):
            xp[pl.ds(pl.multiple_of(t * TILE, TILE), TILE), k * XC:(k + 1) * XC] = stages[k % 2][table_ref[t]]
            return carry

        lax.fori_loop(0, rows // TILE, tile, 0)

    def multiply(b, k):
        s = lax.rem(b, 2)
        prod = jnp.dot(xp[:, k * KC:(k + 1) * KC], wbuf[s, k * KC:(k + 1) * KC, :], preferred_element_type=jnp.float32)
        for h in range(2):
            piece = prod[:, h * HB:(h + 1) * HB]
            if k == 0:
                part[s, h] = piece
            else:
                part[s, h] = part[s, h] + piece

    def step(i, carry):
        @pl.when(i < blocks)
        def _():
            @pl.when(i + 1 < blocks)
            def _():
                w_copy(i + 1).start()

            w_copy(i).wait()
            for k in range(nk - 1):
                multiply(i, k)

        @pl.when(jnp.logical_and(i >= 1, i - 1 < blocks))
        def _():
            b = i - 1
            s, q = lax.rem(b, 2), lax.rem(b, 4)
            copy_a(b).wait()
            there = pl.ds(pl.multiple_of((1 - chip) * half, 8), half)
            here = pl.ds(pl.multiple_of(chip * half, 8), half)
            sb[q] = part[s, core, there, :] + ra[s, there, :]
            so[q] = part[s, core, here, :] + ra[s, here, :]
            copy_b(b).start()

        @pl.when(jnp.logical_and(i >= 3, i - 3 < blocks))
        def _():
            b = i - 3
            copy_b(b).wait()
            out[lax.rem(b, 8), core, chip] = (so[lax.rem(b, 4)] + rb[lax.rem(b, 8)]).astype(out.dtype)
            copy_c(b).start()
            copy_e(b).start()

        @pl.when(jnp.logical_and(i >= 5, i - 5 < blocks))
        def _():
            b = i - 5
            copy_c(b).wait()
            copy_d(b).start()

        @pl.when(jnp.logical_and(i >= 6, i - 6 < blocks))
        def _():
            b = i - 6
            copy_e(b).wait()
            copy_d(b).wait()
            copy_o(b).start()

        @pl.when(jnp.logical_and(i >= 7, i - 7 < blocks))
        def _():
            copy_o(i - 7).wait()

        @pl.when(i < blocks)
        def _():
            multiply(i, nk - 1)
            copy_a(i).start()

        return carry

    lax.fori_loop(0, blocks + LAST, step, 0)


def unpack_kernel(rows, per, lens_ref, p_ref, y_ref):
    slots = lens_ref.shape[0]
    tokens = y_ref.shape[0]
    slot_tiles = tokens // slots // TILE
    half = rows // 2
    offs, _ = tile_offsets(lens_ref, slots)
    for s in range(slots):
        def tile(t, carry, s=s):
            length = lens_ref[s]
            row = t * TILE + lax.broadcasted_iota(jnp.int32, (TILE, HB), 0)
            keep = row < length
            at = jnp.minimum(offs[s] + t, rows // TILE - 1)
            at = pl.multiple_of(at * TILE, TILE)
            target = pl.multiple_of((s * slot_tiles + t) * TILE, TILE)
            for j in range(per):
                for h in range(2):
                    piece = p_ref[j, h, pl.ds(at, TILE), :]
                    piece = jnp.where(keep, piece, jnp.zeros_like(piece))
                    y_ref[pl.ds(target, TILE), (2 * j + h) * HB:(2 * j + h + 1) * HB] = piece
            return carry

        lax.fori_loop(0, slot_tiles, tile, 0)


def branch(index, rows, x_loc, w_loc, lengths, table):
    tokens, depth = x_loc.shape
    cols = w_loc.shape[1]
    blocks = cols // NB
    half = rows // 2
    f32, bf16 = jnp.float32, x_loc.dtype
    dma = pltpu.SemaphoreType.DMA
    packed = pl.pallas_call(
        functools.partial(fused_kernel, rows),
        out_shape=jax.ShapeDtypeStruct((blocks, 2, 2, half, HB), bf16),
        in_specs=[pl.BlockSpec(memory_space=pltpu.SMEM), pl.BlockSpec(memory_space=pl.ANY), pl.BlockSpec(memory_space=pl.ANY)],
        out_specs=pl.BlockSpec(memory_space=pl.ANY),
        scratch_shapes=[
            pltpu.VMEM((rows, depth), bf16),
            pltpu.VMEM((tokens // TILE, TILE, XC), bf16),
            pltpu.VMEM((tokens // TILE, TILE, XC), bf16),
            pltpu.VMEM((2, depth, NB), bf16),
            pltpu.VMEM((2, 2, rows, HB), f32),
            pltpu.VMEM((2, rows, HB), f32),
            pltpu.VMEM((4, half, HB), f32),
            pltpu.VMEM((4, half, HB), f32),
            pltpu.VMEM((8, half, HB), f32),
            pltpu.VMEM((8, 2, 2, half, HB), bf16),
            dma((2,)), dma((2,)), dma((2,)), dma((2,)), dma((4,)), dma((8,)),
            dma((8,)), dma((8,)), dma((8,)), dma((8,)), dma((8,)), dma((8,)), dma((8,)),
        ],
        compiler_params=pltpu.CompilerParams(collective_id=index, has_side_effects=True, vmem_limit_bytes=66_000_000),
        cost_estimate=pl.CostEstimate(flops=2 * rows * depth * cols, bytes_accessed=2 * depth * cols, transcendentals=0),
        name=f"fused_{rows}",
    )(table, x_loc.reshape(tokens // TILE, TILE, depth), w_loc)
    packed = packed.reshape(blocks, 2, rows, HB)
    per = 4
    return pl.pallas_call(
        functools.partial(unpack_kernel, rows, per),
        out_shape=jax.ShapeDtypeStruct((tokens, cols), bf16),
        grid_spec=pltpu.PrefetchScalarGridSpec(
            num_scalar_prefetch=1,
            grid=(blocks // per,),
            in_specs=[pl.BlockSpec((per, 2, rows, HB), lambda g, lens: (g, 0, 0, 0))],
            out_specs=pl.BlockSpec((tokens, per * NB), lambda g, lens: (0, g)),
        ),
        cost_estimate=pl.CostEstimate(flops=0, bytes_accessed=2 * (rows + tokens) * cols, transcendentals=0),
        name=f"unpack_{rows}",
    )(lengths, packed)


def solution(mesh):
    def local_part(x_loc, w_loc, lengths):
        tokens, slots = x_loc.shape[0], lengths.shape[0]
        slot_tiles = tokens // slots // TILE
        tiles = (lengths + TILE - 1) // TILE
        ends = jnp.cumsum(tiles)
        place = jnp.arange(BUCKETS[-1] // TILE, dtype=jnp.int32)
        slot = jnp.minimum(jnp.sum((place[:, None] >= ends[None, :]).astype(jnp.int32), axis=1), slots - 1)
        first = jnp.sum(jnp.where(jnp.arange(slots)[None, :] < slot[:, None], tiles[None, :], 0), axis=1)
        table = slot * slot_tiles + jnp.minimum(place - first, slot_tiles - 1)
        index = jnp.sum((jnp.sum(tiles) * TILE > jnp.array(BUCKETS[:-1], jnp.int32)).astype(jnp.int32))
        return lax.switch(index, [functools.partial(branch, j, rows) for j, rows in enumerate(BUCKETS)], x_loc, w_loc, lengths, table)

    return jax.shard_map(local_part, mesh=mesh, in_specs=(P("data", "tp"), P("tp", None), P("data")), out_specs=P("data", None), check_vma=False)
```

```python
import functools

import jax
import jax.numpy as jnp
from jax import lax
from jax.experimental import pallas as pl
from jax.experimental.pallas import tpu as pltpu
from jax.sharding import PartitionSpec as P

MESH = pl.DeviceIdType.MESH
TILE = 16
NB = 256
HB = NB // 2
KC = 3072
BUCKETS = tuple(range(288, 769, 32)) + (784,)
LAST = 7
OFFS, LONE_TILE, LONE_ROW, LONE_SLOT, LONE_SOURCE, MERGE = 50, 54, 55, 56, 57, 64


def fused_kernel(rows, table_ref, x_ref, w_ref, y_ref, xp, stage0, stage1, lone, wbuf, part, ra, sb, so, rb, out,
                 xsem, wsem, send_a, recv_a, send_b, recv_b, send_c, recv_c, send_e, recv_e, send_d, recv_d, osem):
    depth, cols = w_ref.shape
    blocks = cols // NB
    half = rows // 2
    stages = (stage0, stage1)
    me = lax.axis_index("tp")
    core = lax.rem(me, 2)
    chip = me // 2
    sibling = {"tp": me + 1 - 2 * core}
    peer = {"tp": lax.rem(me + 2, 4)}
    nk = depth // KC

    def x_copy(k):
        return pltpu.make_async_copy(x_ref.at[:, :, pl.ds(k * KC, KC)], stages[k % 2], xsem.at[k % 2])

    def w_copy(b, k):
        s = lax.rem(b, 2)
        deep = pl.ds(pl.multiple_of(k * KC, KC), KC)
        return pltpu.make_async_copy(w_ref.at[deep, pl.ds(pl.multiple_of(b * NB, NB), NB)], wbuf.at[s, deep], wsem.at[s, k])

    def remote(src, dst, ssem, rsem, to):
        return pltpu.make_async_remote_copy(src_ref=src, dst_ref=dst, send_sem=ssem, recv_sem=rsem, device_id=to, device_id_type=MESH)

    def copy_a(b):
        s = lax.rem(b, 2)
        return remote(part.at[s, 1 - core], ra.at[s], send_a.at[s], recv_a.at[s], sibling)

    def copy_b(b):
        s, r = lax.rem(b, 4), lax.rem(b, 8)
        return remote(sb.at[s], rb.at[r], send_b.at[s], recv_b.at[r], peer)

    def copy_c(b):
        r = lax.rem(b, 8)
        return remote(out.at[r, core, chip], out.at[r, core, chip], send_c.at[r], recv_c.at[r], peer)

    def copy_e(b):
        r = lax.rem(b, 8)
        return remote(out.at[r, core, chip], out.at[r, core, chip], send_e.at[r], recv_e.at[r], sibling)

    def copy_d(b):
        r = lax.rem(b, 8)
        return remote(out.at[r, core, 1 - chip], out.at[r, core, 1 - chip], send_d.at[r], recv_d.at[r], sibling)

    def copy_o(b):
        r = lax.rem(b, 8)
        return pltpu.make_async_copy(out.at[r], y_ref.at[b], osem.at[r])

    x_copy(0).start()
    w_copy(0, 0).start()
    x_copy(1).start()
    w_copy(0, 1).start()

    barrier = pltpu.get_barrier_semaphore()
    for other in (sibling, peer):
        pl.semaphore_signal(barrier, inc=1, device_id=other, device_id_type=MESH)
    pl.semaphore_wait(barrier, 2)

    row = lax.broadcasted_iota(jnp.int32, (TILE, KC), 0)

    def pack(k):
        stage = stages[k % 2]
        x_copy(k).wait()
        first = stage[table_ref[LONE_SOURCE]][0:1, :].astype(jnp.float32)
        lone[...] = jnp.broadcast_to(first, (TILE, KC)).astype(lone.dtype)

        def tile(t, carry):
            at = pl.ds(pl.multiple_of(t * TILE, TILE), TILE)
            xp[at, k * KC:(k + 1) * KC] = jnp.where(row == table_ref[MERGE + t], lone[...], stage[table_ref[t]])
            return carry

        lax.fori_loop(0, rows // TILE, tile, 0)
        if k + 2 < nk:
            x_copy(k + 2).start()
            w_copy(0, k + 2).start()
        if k == nk - 1:
            for j in range(nk):
                w_copy(1, j).start()

    def exchange(i):
        @pl.when(jnp.logical_and(i >= 1, i - 1 < blocks))
        def _():
            b = i - 1
            s, q = lax.rem(b, 2), lax.rem(b, 4)
            copy_a(b).wait()
            there = pl.ds(pl.multiple_of((1 - chip) * half, 8), half)
            here = pl.ds(pl.multiple_of(chip * half, 8), half)
            sb[q] = part[s, core, there, :] + ra[s, there, :]
            so[q] = part[s, core, here, :] + ra[s, here, :]
            copy_b(b).start()

        @pl.when(jnp.logical_and(i >= 3, i - 3 < blocks))
        def _():
            b = i - 3
            copy_b(b).wait()
            out[lax.rem(b, 8), core, chip] = (so[lax.rem(b, 4)] + rb[lax.rem(b, 8)]).astype(out.dtype)
            copy_c(b).start()
            copy_e(b).start()

        @pl.when(jnp.logical_and(i >= 5, i - 5 < blocks))
        def _():
            copy_c(i - 5).wait()
            copy_d(i - 5).start()

        @pl.when(jnp.logical_and(i >= 6, i - 6 < blocks))
        def _():
            copy_e(i - 6).wait()
            copy_d(i - 6).wait()
            copy_o(i - 6).start()

        @pl.when(jnp.logical_and(i >= 7, i - 7 < blocks))
        def _():
            copy_o(i - 7).wait()

    def step(j, carry):
        i, k = j // nk, lax.rem(j, nk)
        for early in range(nk):
            pl.when(j == early)(functools.partial(pack, early))

        @pl.when(k == 2)
        def _():
            exchange(i)

        @pl.when(i < blocks)
        def _():
            @pl.when(jnp.logical_and(i >= 1, i + 1 < blocks))
            def _():
                w_copy(i + 1, k).start()

            w_copy(i, k).wait()
            s = lax.rem(i, 2)
            deep = pl.ds(pl.multiple_of(k * KC, KC), KC)
            prod = jnp.dot(xp[:, deep], wbuf[s, deep, :], preferred_element_type=jnp.float32)
            for h in range(2):
                part[s, h] = jnp.where(k == 0, 0.0, part[s, h]) + prod[:, h * HB:(h + 1) * HB]

            @pl.when(k == nk - 1)
            def _():
                copy_a(i).start()

        return carry

    lax.fori_loop(0, nk * (blocks + LAST), step, 0)


def unpack_kernel(per, lens_ref, table_ref, p_ref, y_ref):
    slots = lens_ref.shape[0]
    tokens, width = y_ref.shape
    slot_tiles = tokens // slots // TILE
    row = lax.broadcasted_iota(jnp.int32, (TILE, HB), 0)

    def move(source, target, count, length=None):
        source = pl.multiple_of(source * TILE, TILE)
        target = pl.multiple_of(target * TILE, TILE)
        for j in range(width // HB):
            piece = p_ref[j // 2, j % 2, pl.ds(source, count * TILE), :]
            if length is not None:
                piece = jnp.where(row < length, piece, jnp.zeros_like(piece))
            y_ref[pl.ds(target, count * TILE), j * HB:(j + 1) * HB] = piece

    for s in range(slots):
        merged = jnp.logical_and(table_ref[LONE_TILE] >= 0, table_ref[LONE_SLOT] == s)
        length = jnp.where(merged, 0, lens_ref[s])
        full = length // TILE
        source, target = table_ref[OFFS + s], s * slot_tiles

        def four(t, carry, source=source, target=target):
            move(source + 4 * t, target + 4 * t, 4)
            return carry

        def single(t, carry, source=source, target=target):
            move(source + t, target + t, 1)
            return carry

        lax.fori_loop(0, full // 4, four, 0)
        lax.fori_loop(full // 4 * 4, full, single, 0)

        @pl.when(full * TILE < length)
        def _(source=source, target=target, full=full, length=length):
            move(source + full, target + full, 1, length - full * TILE)

        def clear(t, carry, target=target):
            at = pl.ds(pl.multiple_of((target + t) * TILE, TILE), TILE)
            y_ref[at, :] = jnp.zeros((TILE, width), y_ref.dtype)
            return carry

        lax.fori_loop((length + TILE - 1) // TILE, slot_tiles, clear, 0)

    @pl.when(table_ref[LONE_TILE] >= 0)
    def _():
        source = pl.multiple_of(table_ref[LONE_TILE] * TILE, TILE)
        target = pl.multiple_of(table_ref[LONE_SLOT] * slot_tiles * TILE, TILE)
        for j in range(width // HB):
            piece = p_ref[j // 2, j % 2, pl.ds(source, TILE), :].astype(jnp.float32)
            line = jnp.sum(jnp.where(row == table_ref[LONE_ROW], piece, 0.0), axis=0, keepdims=True)
            y_ref[pl.ds(target, TILE), j * HB:(j + 1) * HB] = jnp.where(row == 0, line, 0.0).astype(y_ref.dtype)


def branch(index, rows, x_loc, w_loc, lengths, table):
    tokens, depth = x_loc.shape
    cols = w_loc.shape[1]
    blocks = cols // NB
    half = rows // 2
    f32, bf16 = jnp.float32, x_loc.dtype
    dma = pltpu.SemaphoreType.DMA
    packed = pl.pallas_call(
        functools.partial(fused_kernel, rows),
        out_shape=jax.ShapeDtypeStruct((blocks, 2, 2, half, HB), bf16),
        in_specs=[pl.BlockSpec(memory_space=pltpu.SMEM), pl.BlockSpec(memory_space=pl.ANY), pl.BlockSpec(memory_space=pl.ANY)],
        out_specs=pl.BlockSpec(memory_space=pl.ANY),
        scratch_shapes=[
            pltpu.VMEM((rows, depth), bf16),
            pltpu.VMEM((tokens // TILE, TILE, KC), bf16),
            pltpu.VMEM((tokens // TILE, TILE, KC), bf16),
            pltpu.VMEM((TILE, KC), bf16),
            pltpu.VMEM((2, depth, NB), bf16),
            pltpu.VMEM((2, 2, rows, HB), f32),
            pltpu.VMEM((2, rows, HB), f32),
            pltpu.VMEM((4, half, HB), f32),
            pltpu.VMEM((4, half, HB), f32),
            pltpu.VMEM((8, half, HB), f32),
            pltpu.VMEM((8, 2, 2, half, HB), bf16),
            dma((2,)), dma((2, depth // KC)), dma((2,)), dma((2,)), dma((4,)), dma((8,)),
            dma((8,)), dma((8,)), dma((8,)), dma((8,)), dma((8,)), dma((8,)), dma((8,)),
        ],
        compiler_params=pltpu.CompilerParams(collective_id=index, has_side_effects=True, vmem_limit_bytes=66_000_000),
        cost_estimate=pl.CostEstimate(flops=2 * rows * depth * cols, bytes_accessed=2 * depth * cols, transcendentals=0),
        name=f"fused_{rows}",
    )(table, x_loc.reshape(tokens // TILE, TILE, depth), w_loc)
    packed = packed.reshape(blocks, 2, rows, HB)
    per = 4
    return pl.pallas_call(
        functools.partial(unpack_kernel, per),
        out_shape=jax.ShapeDtypeStruct((tokens, cols), bf16),
        grid_spec=pltpu.PrefetchScalarGridSpec(
            num_scalar_prefetch=2,
            grid=(blocks // per,),
            in_specs=[pl.BlockSpec((per, 2, rows, HB), lambda g, lens, table: (g, 0, 0, 0))],
            out_specs=pl.BlockSpec((tokens, per * NB), lambda g, lens, table: (0, g)),
        ),
        cost_estimate=pl.CostEstimate(flops=0, bytes_accessed=2 * (rows + tokens) * cols, transcendentals=0),
        name=f"unpack_{rows}",
    )(lengths, table, packed)


def make_table(lengths, tokens):
    slots = lengths.shape[0]
    slot_tiles = tokens // slots // TILE
    lens = [lengths[s] for s in range(slots)]
    lone = jnp.int32(slots - 1)
    for s in reversed(range(slots - 1)):
        lone = jnp.where(lens[s] == 1, s, lone)
    rest = [lens[s] % TILE for s in range(slots)]
    host = jnp.int32(-1)
    for s in reversed(range(slots)):
        host = jnp.where((lone != s) & (rest[s] != 0), s, host)
    merged = host >= 0
    offs, total = [], jnp.int32(0)
    lone_tile, lone_row = jnp.int32(-1), jnp.int32(-1)
    for s in range(slots):
        offs.append(total)
        tiles = jnp.where(merged & (lone == s), 0, (lens[s] + TILE - 1) // TILE)
        total = total + tiles
        lone_tile = jnp.where(host == s, total - 1, lone_tile)
        lone_row = jnp.where(host == s, rest[s], lone_row)
    place = jnp.arange(128, dtype=jnp.int32)
    table = place
    for s in range(1, slots):
        table = jnp.where(place >= offs[s], s * slot_tiles + jnp.minimum(place - offs[s], slot_tiles - 1), table)
    table = jnp.where(place < total, table, 0)
    for s in range(slots):
        table = jnp.where(place == OFFS + s, offs[s], table)
    for at, value in ((LONE_TILE, lone_tile), (LONE_ROW, lone_row), (LONE_SLOT, lone), (LONE_SOURCE, lone * slot_tiles)):
        table = jnp.where(place == at, value, table)
    table = jnp.where(place >= MERGE, jnp.where(place - MERGE == lone_tile, lone_row, -1), table)
    return table, total


def solution(mesh):
    def local_part(x_loc, w_loc, lengths):
        table, total = make_table(lengths, x_loc.shape[0])
        index = jnp.int32(0)
        for size in BUCKETS[:-1]:
            index = index + (total * TILE > size).astype(jnp.int32)
        return lax.switch(index, [functools.partial(branch, j, rows) for j, rows in enumerate(BUCKETS)], x_loc, w_loc, lengths, table)

    return jax.shard_map(local_part, mesh=mesh, in_specs=(P("data", "tp"), P("tp", None), P("data")), out_specs=P("data", None), check_vma=False)
```

```python
import functools

import jax
import jax.numpy as jnp
from jax import lax
from jax.experimental import pallas as pl
from jax.experimental.pallas import tpu as pltpu
from jax.sharding import PartitionSpec as P

MESH = pl.DeviceIdType.MESH
TILE = 16
NB = 256
HB = NB // 2
KC = 3072
BUCKETS = (352, 416, 448) + tuple(range(480, 673, 16)) + (704, 736, 784)
PER = 2
LAST = 7
OFFS, LONE_TILE, LONE_ROW, LONE_SLOT, LONE_SOURCE, MERGE = 50, 54, 55, 56, 57, 64


def fused_kernel(rows, table_ref, x_ref, w_ref, y_ref, xp, stage0, stage1, lone, wbuf, part, ra, sb, so, rb, out,
                 xsem, wsem, send_a, recv_a, send_b, recv_b, send_c, recv_c, send_e, recv_e, send_d, recv_d, osem):
    depth, cols = w_ref.shape
    blocks = cols // NB
    half = rows // 2
    stages = (stage0, stage1)
    me = lax.axis_index("tp")
    core = lax.rem(me, 2)
    chip = me // 2
    sibling = {"tp": me + 1 - 2 * core}
    peer = {"tp": lax.rem(me + 2, 4)}
    nk = depth // KC

    def x_copy(k):
        return pltpu.make_async_copy(x_ref.at[:, :, pl.ds(k * KC, KC)], stages[k % 2], xsem.at[k % 2])

    def w_copy(b, k):
        s = lax.rem(b, 2)
        deep = pl.ds(pl.multiple_of(k * KC, KC), KC)
        return pltpu.make_async_copy(w_ref.at[deep, pl.ds(pl.multiple_of(b * NB, NB), NB)], wbuf.at[s, deep], wsem.at[s, k])

    def remote(src, dst, ssem, rsem, to):
        return pltpu.make_async_remote_copy(src_ref=src, dst_ref=dst, send_sem=ssem, recv_sem=rsem, device_id=to, device_id_type=MESH)

    def copy_a(b):
        s = lax.rem(b, 2)
        return remote(part.at[s, 1 - core], ra.at[s], send_a.at[s], recv_a.at[s], sibling)

    def copy_b(b):
        s, r = lax.rem(b, 4), lax.rem(b, 8)
        return remote(sb.at[s], rb.at[r], send_b.at[s], recv_b.at[r], peer)

    def copy_c(b):
        r = lax.rem(b, 8)
        return remote(out.at[r, core, chip], out.at[r, core, chip], send_c.at[r], recv_c.at[r], peer)

    def copy_e(b):
        r = lax.rem(b, 8)
        return remote(out.at[r, core, chip], out.at[r, core, chip], send_e.at[r], recv_e.at[r], sibling)

    def copy_d(b):
        r = lax.rem(b, 8)
        return remote(out.at[r, core, 1 - chip], out.at[r, core, 1 - chip], send_d.at[r], recv_d.at[r], sibling)

    def copy_o(b):
        r = lax.rem(b, 8)
        return pltpu.make_async_copy(out.at[r], y_ref.at[b], osem.at[r])

    x_copy(0).start()
    w_copy(0, 0).start()
    x_copy(1).start()
    w_copy(0, 1).start()

    barrier = pltpu.get_barrier_semaphore()
    for other in (sibling, peer):
        pl.semaphore_signal(barrier, inc=1, device_id=other, device_id_type=MESH)
    pl.semaphore_wait(barrier, 2)

    row = lax.broadcasted_iota(jnp.int32, (TILE, KC), 0)

    def pack(k):
        stage = stages[k % 2]
        x_copy(k).wait()
        first = stage[table_ref[LONE_SOURCE]][0:1, :].astype(jnp.float32)
        lone[...] = jnp.broadcast_to(first, (TILE, KC)).astype(lone.dtype)

        def tile(t, carry):
            at = pl.ds(pl.multiple_of(t * TILE, TILE), TILE)
            xp[at, k * KC:(k + 1) * KC] = jnp.where(row + 1 == table_ref[MERGE + t], lone[...], stage[table_ref[t]])
            return carry

        lax.fori_loop(0, rows // TILE, tile, 0)
        if k + 2 < nk:
            x_copy(k + 2).start()
            w_copy(0, k + 2).start()
        if k == nk - 1:
            for j in range(nk):
                w_copy(1, j).start()

    def exchange(i):
        @pl.when(jnp.logical_and(i >= 1, i - 1 < blocks))
        def _():
            b = i - 1
            s, q = lax.rem(b, 2), lax.rem(b, 4)
            copy_a(b).wait()
            there = pl.ds(pl.multiple_of((1 - chip) * half, 8), half)
            here = pl.ds(pl.multiple_of(chip * half, 8), half)
            sb[q] = part[s, core, there, :] + ra[s, there, :]
            so[q] = part[s, core, here, :] + ra[s, here, :]
            copy_b(b).start()

        @pl.when(jnp.logical_and(i >= 3, i - 3 < blocks))
        def _():
            b = i - 3
            copy_b(b).wait()
            out[lax.rem(b, 8), core, chip] = (so[lax.rem(b, 4)] + rb[lax.rem(b, 8)]).astype(out.dtype)
            copy_c(b).start()
            copy_e(b).start()

        @pl.when(jnp.logical_and(i >= 5, i - 5 < blocks))
        def _():
            copy_c(i - 5).wait()
            copy_d(i - 5).start()

        @pl.when(jnp.logical_and(i >= 6, i - 6 < blocks))
        def _():
            copy_e(i - 6).wait()
            copy_d(i - 6).wait()
            copy_o(i - 6).start()

        @pl.when(jnp.logical_and(i >= 7, i - 7 < blocks))
        def _():
            copy_o(i - 7).wait()

    def step(j, carry):
        i, k = j // nk, lax.rem(j, nk)
        for early in range(nk):
            pl.when(j == early)(functools.partial(pack, early))

        @pl.when(k == jnp.where(i == 1, 1, 2))
        def _():
            exchange(i)

        @pl.when(i < blocks)
        def _():
            @pl.when(jnp.logical_and(i >= 1, i + 1 < blocks))
            def _():
                w_copy(i + 1, k).start()

            w_copy(i, k).wait()
            s = lax.rem(i, 2)
            deep = pl.ds(pl.multiple_of(k * KC, KC), KC)
            prod = jnp.dot(xp[:, deep], wbuf[s, deep, :], preferred_element_type=jnp.float32)
            for h in range(2):
                part[s, h] = jnp.where(k == 0, 0.0, part[s, h]) + prod[:, h * HB:(h + 1) * HB]

            @pl.when(k == nk - 1)
            def _():
                copy_a(i).start()

        return carry

    lax.fori_loop(0, nk * (blocks + LAST), step, 0)


def unpack_kernel(lens_ref, table_ref, p_ref, y_ref, packed, spread, isem, osem):
    slots = lens_ref.shape[0]
    chunks, tokens, width = spread.shape
    slot_tiles = tokens // slots // TILE
    row = lax.broadcasted_iota(jnp.int32, (TILE, HB), 0)

    def fetch(c):
        return pltpu.make_async_copy(p_ref.at[pl.ds(c * PER, PER)], packed.at[c], isem.at[c])

    def store(c):
        return pltpu.make_async_copy(spread.at[c], y_ref.at[:, pl.ds(pl.multiple_of(c * width, width), width)], osem.at[c])

    def chunk(c, carry):
        fetch(c).wait()

        def move(source, target, count, length=None):
            source = pl.multiple_of(source * TILE, TILE)
            target = pl.multiple_of(target * TILE, TILE)
            for j in range(width // HB):
                piece = packed[c, j // 2, j % 2, pl.ds(source, count * TILE), :]
                if length is not None:
                    piece = jnp.where(row < length, piece, jnp.zeros_like(piece))
                spread[c, pl.ds(target, count * TILE), j * HB:(j + 1) * HB] = piece

        def clear(target, count):
            at = pl.ds(pl.multiple_of(target * TILE, TILE), count * TILE)
            spread[c, at, :] = jnp.zeros((count * TILE, width), spread.dtype)

        for s in range(slots):
            merged = jnp.logical_and(table_ref[LONE_TILE] > 0, table_ref[LONE_SLOT] == s)
            length = jnp.where(merged, 0, lens_ref[s])
            full = lax.div(length, TILE)
            used = lax.div(length + TILE - 1, TILE)
            source, target = table_ref[OFFS + s], s * slot_tiles
            quads = lax.div(full, 4)
            empty = lax.div(used + 3, 4)

            @pl.loop(0, quads)
            def _(t, source=source, target=target):
                move(source + 4 * t, target + 4 * t, 4)

            @pl.loop(quads * 4, full)
            def _(t, source=source, target=target):
                move(source + t, target + t, 1)

            @pl.when(full < used)
            def _(source=source, target=target, full=full, length=length):
                move(source + full, target + full, 1, length - full * TILE)

            @pl.loop(used, empty * 4)
            def _(t, target=target):
                clear(target + t, 1)

            @pl.loop(empty, slot_tiles // 4)
            def _(t, target=target):
                clear(target + 4 * t, 4)

        @pl.when(table_ref[LONE_TILE] > 0)
        def _():
            source = pl.multiple_of((table_ref[LONE_TILE] - 1) * TILE, TILE)
            target = pl.multiple_of(table_ref[LONE_SLOT] * (slot_tiles * TILE), TILE)
            for j in range(width // HB):
                piece = packed[c, j // 2, j % 2, pl.ds(source, TILE), :].astype(jnp.float32)
                line = jnp.sum(jnp.where(row == table_ref[LONE_ROW], piece, 0.0), axis=0, keepdims=True)
                spread[c, pl.ds(target, TILE), j * HB:(j + 1) * HB] = jnp.where(row == 0, line, 0.0).astype(spread.dtype)

        store(c).start()
        return carry

    for c in range(chunks):
        fetch(c).start()
    lax.fori_loop(0, chunks, chunk, 0)
    for c in range(chunks):
        store(c).wait()


def branch(index, rows, x_loc, w_loc, lengths, table):
    tokens, depth = x_loc.shape
    cols = w_loc.shape[1]
    blocks = cols // NB
    half = rows // 2
    f32, bf16 = jnp.float32, x_loc.dtype
    dma = pltpu.SemaphoreType.DMA
    packed = pl.pallas_call(
        functools.partial(fused_kernel, rows),
        out_shape=jax.ShapeDtypeStruct((blocks, 2, 2, half, HB), bf16),
        in_specs=[pl.BlockSpec(memory_space=pltpu.SMEM), pl.BlockSpec(memory_space=pl.ANY), pl.BlockSpec(memory_space=pl.ANY)],
        out_specs=pl.BlockSpec(memory_space=pl.ANY),
        scratch_shapes=[
            pltpu.VMEM((rows, depth), bf16),
            pltpu.VMEM((tokens // TILE, TILE, KC), bf16),
            pltpu.VMEM((tokens // TILE, TILE, KC), bf16),
            pltpu.VMEM((TILE, KC), bf16),
            pltpu.VMEM((2, depth, NB), bf16),
            pltpu.VMEM((2, 2, rows, HB), f32),
            pltpu.VMEM((2, rows, HB), f32),
            pltpu.VMEM((4, half, HB), f32),
            pltpu.VMEM((4, half, HB), f32),
            pltpu.VMEM((8, half, HB), f32),
            pltpu.VMEM((8, 2, 2, half, HB), bf16),
            dma((2,)), dma((2, depth // KC)), dma((2,)), dma((2,)), dma((4,)), dma((8,)),
            dma((8,)), dma((8,)), dma((8,)), dma((8,)), dma((8,)), dma((8,)), dma((8,)),
        ],
        compiler_params=pltpu.CompilerParams(collective_id=index, has_side_effects=True, vmem_limit_bytes=66_000_000),
        cost_estimate=pl.CostEstimate(flops=2 * rows * depth * cols, bytes_accessed=2 * depth * cols, transcendentals=0),
        name=f"fused_{rows}",
    )(table, x_loc.reshape(tokens // TILE, TILE, depth), w_loc)
    packed = packed.reshape(blocks, 2, rows, HB)
    chunks = blocks // PER
    return pl.pallas_call(
        unpack_kernel,
        out_shape=jax.ShapeDtypeStruct((tokens, cols), bf16),
        in_specs=[pl.BlockSpec(memory_space=pltpu.SMEM), pl.BlockSpec(memory_space=pltpu.SMEM), pl.BlockSpec(memory_space=pl.ANY)],
        out_specs=pl.BlockSpec(memory_space=pl.ANY),
        scratch_shapes=[
            pltpu.VMEM((chunks, PER, 2, rows, HB), bf16),
            pltpu.VMEM((chunks, tokens, PER * NB), bf16),
            dma((chunks,)), dma((chunks,)),
        ],
        compiler_params=pltpu.CompilerParams(vmem_limit_bytes=66_000_000),
        cost_estimate=pl.CostEstimate(flops=0, bytes_accessed=2 * (rows + tokens) * cols, transcendentals=0),
        name=f"unpack_{rows}",
    )(lengths, table, packed)


def make_table(lengths, tokens):
    slots = lengths.shape[0]
    slot_tiles = tokens // slots // TILE
    slot = jnp.arange(slots, dtype=jnp.int32)
    ahead = slot[None, :] < slot[:, None]

    def first(flags):
        return flags & ~jnp.any(ahead & flags[None, :], axis=1)

    lone = first(lengths == 1)
    rest = lax.rem(lengths, TILE)
    free = (rest != 0) & ~lone
    host = first(free)
    merged = lone & jnp.any(free[None, :] & (slot[:, None] >= 0), axis=1)
    tiles = jnp.where(merged, 0, lax.div(lengths + (TILE - 1), TILE))
    offs = jnp.sum(jnp.where(ahead, tiles[None, :], 0), axis=1)
    ends = offs + tiles
    place = jnp.arange(128, dtype=jnp.int32)[:, None]
    cells = jnp.where((place >= offs) & (place < ends), slot * slot_tiles + place - offs, 0)
    cells += jnp.where(place == OFFS + slot, offs, 0)
    cells += jnp.where((place == LONE_TILE) & host, ends, 0)
    cells += jnp.where((place == LONE_ROW) & host, rest, 0)
    cells += jnp.where((place == LONE_SLOT) & lone, slot, 0)
    cells += jnp.where((place == LONE_SOURCE) & lone, slot * slot_tiles, 0)
    cells += jnp.where((place - MERGE == ends - 1) & host, rest + 1, 0)
    return jnp.sum(cells, axis=1), jnp.sum(tiles)


def solution(mesh):
    def local_part(x_loc, w_loc, lengths):
        table, total = make_table(lengths, x_loc.shape[0])
        index = jnp.sum((total * TILE > jnp.array(BUCKETS[:-1], jnp.int32)).astype(jnp.int32))
        return lax.switch(index, [functools.partial(branch, j, rows) for j, rows in enumerate(BUCKETS)], x_loc, w_loc, lengths, table)

    return jax.shard_map(local_part, mesh=mesh, in_specs=(P("data", "tp"), P("tp", None), P("data")), out_specs=P("data", None), check_vma=False)
```

```python
import functools

import jax
import jax.numpy as jnp
from jax import lax
from jax.experimental import pallas as pl
from jax.experimental.pallas import tpu as pltpu
from jax.sharding import PartitionSpec as P

MESH = pl.DeviceIdType.MESH
TILE = 16
NB = 256
HB = NB // 2
KC = 3072
XC = 1536
BUCKETS = (352, 416, 448) + tuple(range(480, 673, 16)) + (704, 736, 784)
PER = 2
LAST = 6
OFFS, LONE_TILE, LONE_ROW, LONE_SLOT, LONE_SOURCE, MERGE = 50, 54, 55, 56, 57, 64


def fused_kernel(rows, table_ref, x_ref, w_ref, y_ref, xp, stage0, stage1, stage2, stage3, lone, wbuf, part, ra, sb, so, rb, out,
                 xsem, wsem, send_a, recv_a, send_b, recv_b, send_c, recv_c, send_e, recv_e, send_d, recv_d, osem):
    depth, cols = w_ref.shape
    blocks = cols // NB
    half = rows // 2
    stages = (stage0, stage1, stage2, stage3)
    ns = len(stages)
    me = lax.axis_index("tp")
    core = lax.rem(me, 2)
    chip = me // 2
    sibling = {"tp": me + 1 - 2 * core}
    peer = {"tp": lax.rem(me + 2, 4)}
    nk = depth // KC
    nx = depth // XC
    per = nx // nk

    def x_copy(n):
        return pltpu.make_async_copy(x_ref.at[:, :, pl.ds(n * XC, XC)], stages[n % ns], xsem.at[n % ns])

    def w_copy(b, k):
        s = lax.rem(b, 2)
        deep = pl.ds(pl.multiple_of(k * KC, KC), KC)
        return pltpu.make_async_copy(w_ref.at[deep, pl.ds(pl.multiple_of(b * NB, NB), NB)], wbuf.at[s, deep], wsem.at[s, k])

    def remote(src, dst, ssem, rsem, to):
        return pltpu.make_async_remote_copy(src_ref=src, dst_ref=dst, send_sem=ssem, recv_sem=rsem, device_id=to, device_id_type=MESH)

    def copy_a(b):
        s = lax.rem(b, 2)
        return remote(part.at[s, 1 - core], ra.at[s], send_a.at[s], recv_a.at[s], sibling)

    def copy_b(b):
        s, r = lax.rem(b, 4), lax.rem(b, 8)
        return remote(sb.at[s], rb.at[r], send_b.at[s], recv_b.at[r], peer)

    def copy_c(b):
        r = lax.rem(b, 8)
        return remote(out.at[r, core, chip], out.at[r, core, chip], send_c.at[r], recv_c.at[r], peer)

    def copy_e(b):
        r = lax.rem(b, 8)
        return remote(out.at[r, core, chip], out.at[r, core, chip], send_e.at[r], recv_e.at[r], sibling)

    def copy_d(b):
        r = lax.rem(b, 8)
        return remote(out.at[r, core, 1 - chip], out.at[r, core, 1 - chip], send_d.at[r], recv_d.at[r], sibling)

    def copy_o(b):
        r = lax.rem(b, 8)
        return pltpu.make_async_copy(out.at[r], y_ref.at[b], osem.at[r])

    for n in range(ns):
        x_copy(n).start()
        if n % per == per - 1:
            w_copy(0, n // per).start()

    barrier = pltpu.get_barrier_semaphore()
    for other in (sibling, peer):
        pl.semaphore_signal(barrier, inc=1, device_id=other, device_id_type=MESH)
    pl.semaphore_wait(barrier, 2)

    row = lax.broadcasted_iota(jnp.int32, (TILE, XC), 0)

    def pack(n):
        stage = stages[n % ns]
        x_copy(n).wait()
        if n == nx - 1:
            for k in range(nk):
                w_copy(1, k).start()
        first = stage[table_ref[LONE_SOURCE]][0:1, :].astype(jnp.float32)
        lone[...] = jnp.broadcast_to(first, (TILE, XC)).astype(lone.dtype)

        def tile(t, carry):
            at = pl.ds(pl.multiple_of(t * TILE, TILE), TILE)
            xp[at, n * XC:(n + 1) * XC] = jnp.where(row + 1 == table_ref[MERGE + t], lone[...], stage[table_ref[t]])
            return carry

        lax.fori_loop(0, rows // TILE, tile, 0)
        if n + ns < nx:
            x_copy(n + ns).start()
            if (n + ns) % per == per - 1:
                w_copy(0, (n + ns) // per).start()

    def pack_for(k):
        for n in range(k * per, (k + 1) * per):
            pack(n)

    def reduce_on(i):
        @pl.when(jnp.logical_and(i >= 1, i - 1 < blocks))
        def _():
            b = i - 1
            s, q = lax.rem(b, 2), lax.rem(b, 4)
            copy_a(b).wait()
            there = pl.ds(pl.multiple_of((1 - chip) * half, 8), half)
            here = pl.ds(pl.multiple_of(chip * half, 8), half)
            sb[q] = part[s, core, there, :] + ra[s, there, :]
            so[q] = part[s, core, here, :] + ra[s, here, :]
            copy_b(b).start()

    def finish(i):
        @pl.when(jnp.logical_and(i >= 2, i - 2 < blocks))
        def _():
            b = i - 2
            copy_b(b).wait()
            out[lax.rem(b, 8), core, chip] = (so[lax.rem(b, 4)] + rb[lax.rem(b, 8)]).astype(out.dtype)
            copy_c(b).start()
            copy_e(b).start()

        @pl.when(jnp.logical_and(i >= 4, i - 4 < blocks))
        def _():
            copy_c(i - 4).wait()
            copy_d(i - 4).start()

        @pl.when(jnp.logical_and(i >= 5, i - 5 < blocks))
        def _():
            copy_e(i - 5).wait()
            copy_d(i - 5).wait()
            copy_o(i - 5).start()

        @pl.when(jnp.logical_and(i >= 6, i - 6 < blocks))
        def _():
            copy_o(i - 6).wait()

    def step(j, carry):
        i, k = j // nk, lax.rem(j, nk)
        for early in range(nk):
            pl.when(j == early)(functools.partial(pack_for, early))

        @pl.when(k == jnp.where(i <= 3, 1, 2))
        def _():
            reduce_on(i)

        @pl.when(k == nk - 1)
        def _():
            finish(i)

        @pl.when(i < blocks)
        def _():
            @pl.when(jnp.logical_and(i >= 1, i + 1 < blocks))
            def _():
                w_copy(i + 1, k).start()

            w_copy(i, k).wait()
            s = lax.rem(i, 2)
            deep = pl.ds(pl.multiple_of(k * KC, KC), KC)
            prod = jnp.dot(xp[:, deep], wbuf[s, deep, :], preferred_element_type=jnp.float32)
            for h in range(2):
                part[s, h] = jnp.where(k == 0, 0.0, part[s, h]) + prod[:, h * HB:(h + 1) * HB]

            @pl.when(k == nk - 1)
            def _():
                copy_a(i).start()

        return carry

    lax.fori_loop(0, nk * (blocks + LAST), step, 0)


def unpack_kernel(lens_ref, table_ref, p_ref, y_ref, packed, spread, isem, osem):
    slots = lens_ref.shape[0]
    chunks, tokens, width = spread.shape
    slot_tiles = tokens // slots // TILE
    row = lax.broadcasted_iota(jnp.int32, (TILE, HB), 0)

    def fetch(c):
        return pltpu.make_async_copy(p_ref.at[pl.ds(c * PER, PER)], packed.at[c], isem.at[c])

    def store(c):
        return pltpu.make_async_copy(spread.at[c], y_ref.at[:, pl.ds(pl.multiple_of(c * width, width), width)], osem.at[c])

    def chunk(c, carry):
        fetch(c).wait()

        def move(source, target, count, length=None):
            source = pl.multiple_of(source * TILE, TILE)
            target = pl.multiple_of(target * TILE, TILE)
            for j in range(width // HB):
                piece = packed[c, j // 2, j % 2, pl.ds(source, count * TILE), :]
                if length is not None:
                    piece = jnp.where(row < length, piece, jnp.zeros_like(piece))
                spread[c, pl.ds(target, count * TILE), j * HB:(j + 1) * HB] = piece

        def clear(target, count):
            at = pl.ds(pl.multiple_of(target * TILE, TILE), count * TILE)
            spread[c, at, :] = jnp.zeros((count * TILE, width), spread.dtype)

        for s in range(slots):
            merged = jnp.logical_and(table_ref[LONE_TILE] > 0, table_ref[LONE_SLOT] == s)
            length = jnp.where(merged, 0, lens_ref[s])
            full = lax.div(length, TILE)
            used = lax.div(length + TILE - 1, TILE)
            source, target = table_ref[OFFS + s], s * slot_tiles
            quads = lax.div(full, 4)
            empty = lax.div(used + 3, 4)

            @pl.loop(0, quads)
            def _(t, source=source, target=target):
                move(source + 4 * t, target + 4 * t, 4)

            @pl.loop(quads * 4, full)
            def _(t, source=source, target=target):
                move(source + t, target + t, 1)

            @pl.when(full < used)
            def _(source=source, target=target, full=full, length=length):
                move(source + full, target + full, 1, length - full * TILE)

            @pl.loop(used, empty * 4)
            def _(t, target=target):
                clear(target + t, 1)

            @pl.loop(empty, slot_tiles // 4)
            def _(t, target=target):
                clear(target + 4 * t, 4)

        @pl.when(table_ref[LONE_TILE] > 0)
        def _():
            source = pl.multiple_of((table_ref[LONE_TILE] - 1) * TILE, TILE)
            target = pl.multiple_of(table_ref[LONE_SLOT] * (slot_tiles * TILE), TILE)
            for j in range(width // HB):
                piece = packed[c, j // 2, j % 2, pl.ds(source, TILE), :].astype(jnp.float32)
                line = jnp.sum(jnp.where(row == table_ref[LONE_ROW], piece, 0.0), axis=0, keepdims=True)
                spread[c, pl.ds(target, TILE), j * HB:(j + 1) * HB] = jnp.where(row == 0, line, 0.0).astype(spread.dtype)

        store(c).start()
        return carry

    for c in range(chunks):
        fetch(c).start()
    lax.fori_loop(0, chunks, chunk, 0)
    for c in range(chunks):
        store(c).wait()


def branch(index, rows, x_loc, w_loc, lengths, table):
    tokens, depth = x_loc.shape
    cols = w_loc.shape[1]
    blocks = cols // NB
    half = rows // 2
    f32, bf16 = jnp.float32, x_loc.dtype
    dma = pltpu.SemaphoreType.DMA
    packed = pl.pallas_call(
        functools.partial(fused_kernel, rows),
        out_shape=jax.ShapeDtypeStruct((blocks, 2, 2, half, HB), bf16),
        in_specs=[pl.BlockSpec(memory_space=pltpu.SMEM), pl.BlockSpec(memory_space=pl.ANY), pl.BlockSpec(memory_space=pl.ANY)],
        out_specs=pl.BlockSpec(memory_space=pl.ANY),
        scratch_shapes=[
            pltpu.VMEM((rows, depth), bf16),
            *[pltpu.VMEM((tokens // TILE, TILE, XC), bf16)] * 4,
            pltpu.VMEM((TILE, XC), bf16),
            pltpu.VMEM((2, depth, NB), bf16),
            pltpu.VMEM((2, 2, rows, HB), f32),
            pltpu.VMEM((2, rows, HB), f32),
            pltpu.VMEM((4, half, HB), f32),
            pltpu.VMEM((4, half, HB), f32),
            pltpu.VMEM((8, half, HB), f32),
            pltpu.VMEM((8, 2, 2, half, HB), bf16),
            dma((4,)), dma((2, depth // KC)), dma((2,)), dma((2,)), dma((4,)), dma((8,)),
            dma((8,)), dma((8,)), dma((8,)), dma((8,)), dma((8,)), dma((8,)), dma((8,)),
        ],
        compiler_params=pltpu.CompilerParams(collective_id=index, has_side_effects=True, vmem_limit_bytes=66_000_000),
        cost_estimate=pl.CostEstimate(flops=2 * rows * depth * cols, bytes_accessed=2 * depth * cols, transcendentals=0),
        name=f"fused_{rows}",
    )(table, x_loc.reshape(tokens // TILE, TILE, depth), w_loc)
    packed = packed.reshape(blocks, 2, rows, HB)
    chunks = blocks // PER
    return pl.pallas_call(
        unpack_kernel,
        out_shape=jax.ShapeDtypeStruct((tokens, cols), bf16),
        in_specs=[pl.BlockSpec(memory_space=pltpu.SMEM), pl.BlockSpec(memory_space=pltpu.SMEM), pl.BlockSpec(memory_space=pl.ANY)],
        out_specs=pl.BlockSpec(memory_space=pl.ANY),
        scratch_shapes=[
            pltpu.VMEM((chunks, PER, 2, rows, HB), bf16),
            pltpu.VMEM((chunks, tokens, PER * NB), bf16),
            dma((chunks,)), dma((chunks,)),
        ],
        compiler_params=pltpu.CompilerParams(vmem_limit_bytes=66_000_000),
        cost_estimate=pl.CostEstimate(flops=0, bytes_accessed=2 * (rows + tokens) * cols, transcendentals=0),
        name=f"unpack_{rows}",
    )(lengths, table, packed)


def table_kernel(tokens, lens_ref, table_ref, index_ref):
    slots = lens_ref.shape[0]
    slot_tiles = tokens // slots // TILE
    lens = [lens_ref[s] for s in range(slots)]
    lone = jnp.int32(slots - 1)
    for s in reversed(range(slots - 1)):
        lone = jnp.where(lens[s] == 1, s, lone)
    rest = [lax.rem(lens[s], TILE) for s in range(slots)]
    host = jnp.int32(-1)
    for s in reversed(range(slots)):
        host = jnp.where(jnp.logical_and(lone != s, rest[s] != 0), s, host)
    offs, total = [], jnp.int32(0)
    lone_tile, lone_row = jnp.int32(0), jnp.int32(0)
    for s in range(slots):
        offs.append(total)
        tiles = jnp.where(jnp.logical_and(host >= 0, lone == s), 0, lax.div(lens[s] + (TILE - 1), TILE))
        total = total + tiles
        lone_tile = jnp.where(host == s, total, lone_tile)
        lone_row = jnp.where(host == s, rest[s], lone_row)

    def tile(t, carry):
        source = t
        for s in range(1, slots):
            source = jnp.where(t >= offs[s], s * slot_tiles + t - offs[s], source)
        table_ref[t] = jnp.where(t < total, source, 0)
        table_ref[MERGE + t] = jnp.where(t + 1 == lone_tile, lone_row + 1, 0)
        return carry

    lax.fori_loop(0, OFFS, tile, 0)
    for s in range(slots):
        table_ref[OFFS + s] = offs[s]
    table_ref[LONE_TILE] = lone_tile
    table_ref[LONE_ROW] = lone_row
    table_ref[LONE_SLOT] = lone
    table_ref[LONE_SOURCE] = lone * slot_tiles
    index = jnp.int32(0)
    for size in BUCKETS[:-1]:
        index = index + (total * TILE > size).astype(jnp.int32)
    index_ref[0] = index


def make_table(lengths, tokens):
    smem = pl.BlockSpec(memory_space=pltpu.SMEM)
    return pl.pallas_call(
        functools.partial(table_kernel, tokens),
        out_shape=(jax.ShapeDtypeStruct((128,), jnp.int32), jax.ShapeDtypeStruct((1,), jnp.int32)),
        in_specs=[smem],
        out_specs=(smem, smem),
        name="table",
    )(lengths)


def solution(mesh):
    def local_part(x_loc, w_loc, lengths):
        table, index = make_table(lengths, x_loc.shape[0])
        return lax.switch(index[0], [functools.partial(branch, j, rows) for j, rows in enumerate(BUCKETS)], x_loc, w_loc, lengths, table)

    return jax.shard_map(local_part, mesh=mesh, in_specs=(P("data", "tp"), P("tp", None), P("data")), out_specs=P("data", None), check_vma=False)
```

```python
import functools

import jax
import jax.numpy as jnp
from jax import lax
from jax.experimental import pallas as pl
from jax.experimental.pallas import tpu as pltpu
from jax.sharding import PartitionSpec as P

MESH = pl.DeviceIdType.MESH
TILE = 16
NB = 256
HB = NB // 2
KC = 3072
XC = 1536
BUCKETS = (352, 416, 448) + tuple(range(480, 673, 16)) + (704, 736, 784)
PER = 4
LAST = 6
OFFS, LONE_TILE, LONE_ROW, LONE_SLOT, LONE_SOURCE, MERGE = 50, 54, 55, 56, 57, 64


def fused_kernel(rows, table_ref, x_ref, w_ref, y_ref, xp, stage0, stage1, stage2, stage3, lone, wbuf, part, ra, sb, so, rb, out,
                 xsem, wsem, send_a, recv_a, send_b, recv_b, send_c, recv_c, send_e, recv_e, send_d, recv_d, osem):
    depth, cols = w_ref.shape
    blocks = cols // NB
    half = rows // 2
    stages = (stage0, stage1, stage2, stage3)
    ns = len(stages)
    me = lax.axis_index("tp")
    core = lax.rem(me, 2)
    chip = me // 2
    sibling = {"tp": me + 1 - 2 * core}
    peer = {"tp": lax.rem(me + 2, 4)}
    nk = depth // KC
    nx = depth // XC
    per = nx // nk

    def x_copy(n):
        return pltpu.make_async_copy(x_ref.at[:, :, pl.ds(n * XC, XC)], stages[n % ns], xsem.at[n % ns])

    def w_copy(b, k):
        s = lax.rem(b, 2)
        deep = pl.ds(pl.multiple_of(k * KC, KC), KC)
        return pltpu.make_async_copy(w_ref.at[deep, pl.ds(pl.multiple_of(b * NB, NB), NB)], wbuf.at[s, deep], wsem.at[s, k])

    def remote(src, dst, ssem, rsem, to):
        return pltpu.make_async_remote_copy(src_ref=src, dst_ref=dst, send_sem=ssem, recv_sem=rsem, device_id=to, device_id_type=MESH)

    def copy_a(b):
        s = lax.rem(b, 2)
        return remote(part.at[s, 1 - core], ra.at[s], send_a.at[s], recv_a.at[s], sibling)

    def copy_b(b):
        s, r = lax.rem(b, 4), lax.rem(b, 8)
        return remote(sb.at[s], rb.at[r], send_b.at[s], recv_b.at[r], peer)

    def copy_c(b):
        r = lax.rem(b, 8)
        return remote(out.at[r, core, chip], out.at[r, core, chip], send_c.at[r], recv_c.at[r], peer)

    def copy_e(b):
        r = lax.rem(b, 8)
        return remote(out.at[r, core, chip], out.at[r, core, chip], send_e.at[r], recv_e.at[r], sibling)

    def copy_d(b):
        r = lax.rem(b, 8)
        return remote(out.at[r, core, 1 - chip], out.at[r, core, 1 - chip], send_d.at[r], recv_d.at[r], sibling)

    def copy_o(b):
        r = lax.rem(b, 8)
        return pltpu.make_async_copy(out.at[r], y_ref.at[b], osem.at[r])

    for n in range(ns):
        x_copy(n).start()
        if n % per == per - 1:
            w_copy(0, n // per).start()

    barrier = pltpu.get_barrier_semaphore()
    for other in (sibling, peer):
        pl.semaphore_signal(barrier, inc=1, device_id=other, device_id_type=MESH)
    pl.semaphore_wait(barrier, 2)

    row = lax.broadcasted_iota(jnp.int32, (TILE, XC), 0)

    def pack(n):
        stage = stages[n % ns]
        x_copy(n).wait()
        if n == nx - 1:
            for k in range(nk):
                w_copy(1, k).start()
        first = stage[table_ref[LONE_SOURCE]][0:1, :].astype(jnp.float32)
        lone[...] = jnp.broadcast_to(first, (TILE, XC)).astype(lone.dtype)

        def tile(t, carry):
            at = pl.ds(pl.multiple_of(t * TILE, TILE), TILE)
            xp[at, n * XC:(n + 1) * XC] = jnp.where(row + 1 == table_ref[MERGE + t], lone[...], stage[table_ref[t]])
            return carry

        lax.fori_loop(0, rows // TILE, tile, 0)
        if n + ns < nx:
            x_copy(n + ns).start()
            if (n + ns) % per == per - 1:
                w_copy(0, (n + ns) // per).start()

    def pack_for(k):
        for n in range(k * per, (k + 1) * per):
            pack(n)

    def reduce_on(i):
        @pl.when(jnp.logical_and(i >= 1, i - 1 < blocks))
        def _():
            b = i - 1
            s, q = lax.rem(b, 2), lax.rem(b, 4)
            copy_a(b).wait()
            there = pl.ds(pl.multiple_of((1 - chip) * half, 8), half)
            here = pl.ds(pl.multiple_of(chip * half, 8), half)
            sb[q] = part[s, core, there, :] + ra[s, there, :]
            so[q] = part[s, core, here, :] + ra[s, here, :]
            copy_b(b).start()

    def finish(i):
        @pl.when(jnp.logical_and(i >= 2, i - 2 < blocks))
        def _():
            b = i - 2
            copy_b(b).wait()
            out[lax.rem(b, 8), core, chip] = (so[lax.rem(b, 4)] + rb[lax.rem(b, 8)]).astype(out.dtype)
            copy_c(b).start()
            copy_e(b).start()

        @pl.when(jnp.logical_and(i >= 4, i - 4 < blocks))
        def _():
            copy_c(i - 4).wait()
            copy_d(i - 4).start()

        @pl.when(jnp.logical_and(i >= 5, i - 5 < blocks))
        def _():
            copy_e(i - 5).wait()
            copy_d(i - 5).wait()
            copy_o(i - 5).start()

        @pl.when(jnp.logical_and(i >= 6, i - 6 < blocks))
        def _():
            copy_o(i - 6).wait()

    def step(j, carry):
        i, k = j // nk, lax.rem(j, nk)
        for early in range(nk):
            pl.when(j == early)(functools.partial(pack_for, early))

        @pl.when(k == jnp.where(i <= 3, 1, 2))
        def _():
            reduce_on(i)

        @pl.when(k == nk - 1)
        def _():
            finish(i)

        @pl.when(i < blocks)
        def _():
            @pl.when(jnp.logical_and(i >= 1, i + 1 < blocks))
            def _():
                w_copy(i + 1, k).start()

            w_copy(i, k).wait()
            s = lax.rem(i, 2)
            deep = pl.ds(pl.multiple_of(k * KC, KC), KC)
            split = rows // (2 * TILE) * TILE
            for part_rows in (slice(0, split), slice(split, rows)):
                prod = jnp.dot(xp[part_rows, deep], wbuf[s, deep, :], preferred_element_type=jnp.float32)
                for h in range(2):
                    part[s, h, part_rows] = jnp.where(k == 0, 0.0, part[s, h, part_rows]) + prod[:, h * HB:(h + 1) * HB]

            @pl.when(k == nk - 1)
            def _():
                copy_a(i).start()

        return carry

    lax.fori_loop(0, nk * (blocks + LAST), step, 0)


def unpack_kernel(lens_ref, table_ref, p_ref, y_ref, packed, spread, isem, osem):
    slots = lens_ref.shape[0]
    chunks, tokens, width = spread.shape
    slot_tiles = tokens // slots // TILE
    row = lax.broadcasted_iota(jnp.int32, (TILE, HB), 0)

    def fetch(c):
        return pltpu.make_async_copy(p_ref.at[pl.ds(c * PER, PER)], packed.at[c], isem.at[c])

    def store(c):
        return pltpu.make_async_copy(spread.at[c], y_ref.at[:, pl.ds(pl.multiple_of(c * width, width), width)], osem.at[c])

    def chunk(c, carry):
        fetch(c).wait()

        def move(source, target, count, length=None):
            source = pl.multiple_of(source * TILE, TILE)
            target = pl.multiple_of(target * TILE, TILE)
            for j in range(width // HB):
                piece = packed[c, j // 2, j % 2, pl.ds(source, count * TILE), :]
                if length is not None:
                    piece = jnp.where(row < length, piece, jnp.zeros_like(piece))
                spread[c, pl.ds(target, count * TILE), j * HB:(j + 1) * HB] = piece

        def clear(target, count):
            at = pl.ds(pl.multiple_of(target * TILE, TILE), count * TILE)
            spread[c, at, :] = jnp.zeros((count * TILE, width), spread.dtype)

        @pl.loop(0, slots)
        def _(s):
            merged = jnp.logical_and(table_ref[LONE_TILE] > 0, table_ref[LONE_SLOT] == s)
            length = jnp.where(merged, 0, lens_ref[s])
            full = lax.div(length, TILE)
            used = lax.div(length + TILE - 1, TILE)
            source, target = table_ref[OFFS + s], s * slot_tiles
            quads = lax.div(full, 4)
            empty = lax.div(used + 3, 4)

            @pl.loop(0, quads)
            def _(t):
                move(source + 4 * t, target + 4 * t, 4)

            @pl.loop(quads * 4, full)
            def _(t):
                move(source + t, target + t, 1)

            @pl.when(full < used)
            def _():
                move(source + full, target + full, 1, length - full * TILE)

            @pl.loop(used, empty * 4)
            def _(t):
                clear(target + t, 1)

            @pl.loop(empty, slot_tiles // 4)
            def _(t):
                clear(target + 4 * t, 4)

        @pl.when(table_ref[LONE_TILE] > 0)
        def _():
            source = pl.multiple_of((table_ref[LONE_TILE] - 1) * TILE, TILE)
            target = pl.multiple_of(table_ref[LONE_SLOT] * (slot_tiles * TILE), TILE)
            for j in range(width // HB):
                piece = packed[c, j // 2, j % 2, pl.ds(source, TILE), :].astype(jnp.float32)
                line = jnp.sum(jnp.where(row == table_ref[LONE_ROW], piece, 0.0), axis=0, keepdims=True)
                spread[c, pl.ds(target, TILE), j * HB:(j + 1) * HB] = jnp.where(row == 0, line, 0.0).astype(spread.dtype)

        store(c).start()
        return carry

    for c in range(chunks):
        fetch(c).start()
    lax.fori_loop(0, chunks, chunk, 0)
    for c in range(chunks):
        store(c).wait()


def branch(index, rows, x_loc, w_loc, lengths, table):
    tokens, depth = x_loc.shape
    cols = w_loc.shape[1]
    blocks = cols // NB
    half = rows // 2
    f32, bf16 = jnp.float32, x_loc.dtype
    dma = pltpu.SemaphoreType.DMA
    packed = pl.pallas_call(
        functools.partial(fused_kernel, rows),
        out_shape=jax.ShapeDtypeStruct((blocks, 2, 2, half, HB), bf16),
        in_specs=[pl.BlockSpec(memory_space=pltpu.SMEM), pl.BlockSpec(memory_space=pl.ANY), pl.BlockSpec(memory_space=pl.ANY)],
        out_specs=pl.BlockSpec(memory_space=pl.ANY),
        scratch_shapes=[
            pltpu.VMEM((rows, depth), bf16),
            *[pltpu.VMEM((tokens // TILE, TILE, XC), bf16)] * 4,
            pltpu.VMEM((TILE, XC), bf16),
            pltpu.VMEM((2, depth, NB), bf16),
            pltpu.VMEM((2, 2, rows, HB), f32),
            pltpu.VMEM((2, rows, HB), f32),
            pltpu.VMEM((4, half, HB), f32),
            pltpu.VMEM((4, half, HB), f32),
            pltpu.VMEM((8, half, HB), f32),
            pltpu.VMEM((8, 2, 2, half, HB), bf16),
            dma((4,)), dma((2, depth // KC)), dma((2,)), dma((2,)), dma((4,)), dma((8,)),
            dma((8,)), dma((8,)), dma((8,)), dma((8,)), dma((8,)), dma((8,)), dma((8,)),
        ],
        compiler_params=pltpu.CompilerParams(collective_id=index, has_side_effects=True, vmem_limit_bytes=66_000_000),
        cost_estimate=pl.CostEstimate(flops=2 * rows * depth * cols, bytes_accessed=2 * depth * cols, transcendentals=0),
        name=f"fused_{rows}",
    )(table, x_loc.reshape(tokens // TILE, TILE, depth), w_loc)
    packed = packed.reshape(blocks, 2, rows, HB)
    chunks = blocks // PER
    return pl.pallas_call(
        unpack_kernel,
        out_shape=jax.ShapeDtypeStruct((tokens, cols), bf16),
        in_specs=[pl.BlockSpec(memory_space=pltpu.SMEM), pl.BlockSpec(memory_space=pltpu.SMEM), pl.BlockSpec(memory_space=pl.ANY)],
        out_specs=pl.BlockSpec(memory_space=pl.ANY),
        scratch_shapes=[
            pltpu.VMEM((chunks, PER, 2, rows, HB), bf16),
            pltpu.VMEM((chunks, tokens, PER * NB), bf16),
            dma((chunks,)), dma((chunks,)),
        ],
        compiler_params=pltpu.CompilerParams(vmem_limit_bytes=66_000_000),
        cost_estimate=pl.CostEstimate(flops=0, bytes_accessed=2 * (rows + tokens) * cols, transcendentals=0),
        name=f"unpack_{rows}",
    )(lengths, table, packed)


def table_kernel(tokens, lens_ref, table_ref, index_ref):
    slots = lens_ref.shape[0]
    slot_tiles = tokens // slots // TILE
    lens = [lens_ref[s] for s in range(slots)]
    lone = jnp.int32(slots - 1)
    for s in reversed(range(slots - 1)):
        lone = jnp.where(lens[s] == 1, s, lone)
    rest = [lax.rem(lens[s], TILE) for s in range(slots)]
    host = jnp.int32(-1)
    for s in reversed(range(slots)):
        host = jnp.where(jnp.logical_and(lone != s, rest[s] != 0), s, host)
    offs, total = [], jnp.int32(0)
    lone_tile, lone_row = jnp.int32(0), jnp.int32(0)
    for s in range(slots):
        offs.append(total)
        tiles = jnp.where(jnp.logical_and(host >= 0, lone == s), 0, lax.div(lens[s] + (TILE - 1), TILE))
        total = total + tiles
        lone_tile = jnp.where(host == s, total, lone_tile)
        lone_row = jnp.where(host == s, rest[s], lone_row)

    def tile(t, carry):
        source = t
        for s in range(1, slots):
            source = jnp.where(t >= offs[s], s * slot_tiles + t - offs[s], source)
        table_ref[t] = jnp.where(t < total, source, 0)
        table_ref[MERGE + t] = jnp.where(t + 1 == lone_tile, lone_row + 1, 0)
        return carry

    lax.fori_loop(0, OFFS, tile, 0)
    for s in range(slots):
        table_ref[OFFS + s] = offs[s]
    table_ref[LONE_TILE] = lone_tile
    table_ref[LONE_ROW] = lone_row
    table_ref[LONE_SLOT] = lone
    table_ref[LONE_SOURCE] = lone * slot_tiles
    index = jnp.int32(0)
    for size in BUCKETS[:-1]:
        index = index + (total * TILE > size).astype(jnp.int32)
    index_ref[0] = index


def make_table(lengths, tokens):
    smem = pl.BlockSpec(memory_space=pltpu.SMEM)
    return pl.pallas_call(
        functools.partial(table_kernel, tokens),
        out_shape=(jax.ShapeDtypeStruct((128,), jnp.int32), jax.ShapeDtypeStruct((1,), jnp.int32)),
        in_specs=[smem],
        out_specs=(smem, smem),
        name="table",
    )(lengths)


def solution(mesh):
    def local_part(x_loc, w_loc, lengths):
        table, index = make_table(lengths, x_loc.shape[0])
        return lax.switch(index[0], [functools.partial(branch, j, rows) for j, rows in enumerate(BUCKETS)], x_loc, w_loc, lengths, table)

    return jax.shard_map(local_part, mesh=mesh, in_specs=(P("data", "tp"), P("tp", None), P("data")), out_specs=P("data", None), check_vma=False)
```

```python
import functools

import jax
import jax.numpy as jnp
from jax import lax
from jax.experimental import pallas as pl
from jax.experimental.pallas import tpu as pltpu
from jax.sharding import PartitionSpec as P

MESH = pl.DeviceIdType.MESH
TILE = 16
NB = 256
HB = NB // 2
KC = 3072
XC = 1536
BUCKETS = (352, 416, 448) + tuple(range(480, 673, 16)) + (704, 736, 784)
PER = 4
LAST = 5
OFFS, LONE_TILE, LONE_ROW, LONE_SLOT, LONE_SOURCE, MERGE = 50, 54, 55, 56, 57, 64


def fused_kernel(rows, table_ref, x_ref, w_ref, out, *scratch):
    (xp, lone, wbuf, part, ra, sb, so, rb, xsem, wsem, send_a, recv_a, send_b, recv_b, send_c, recv_c, send_e, recv_e,
     send_d, recv_d, *stages) = scratch
    depth, cols = w_ref.shape
    blocks = cols // NB
    half = rows // 2
    ns = len(stages)
    me = lax.axis_index("tp")
    core = lax.rem(me, 2)
    chip = me // 2
    sibling = {"tp": me + 1 - 2 * core}
    peer = {"tp": lax.rem(me + 2, 4)}
    nk = depth // KC
    nx = depth // XC
    per = nx // nk

    def x_copy(n):
        return pltpu.make_async_copy(x_ref.at[:, :, pl.ds(n * XC, XC)], stages[n % ns], xsem.at[n % ns])

    def w_copy(b, k):
        s = lax.rem(b, 2)
        deep = pl.ds(pl.multiple_of(k * KC, KC), KC)
        return pltpu.make_async_copy(w_ref.at[deep, pl.ds(pl.multiple_of(b * NB, NB), NB)], wbuf.at[s, deep], wsem.at[s, k])

    def remote(src, dst, ssem, rsem, to):
        return pltpu.make_async_remote_copy(src_ref=src, dst_ref=dst, send_sem=ssem, recv_sem=rsem, device_id=to, device_id_type=MESH)

    def copy_a(b):
        s = lax.rem(b, 2)
        return remote(part.at[s, 1 - core], ra.at[s], send_a.at[s], recv_a.at[s], sibling)

    def copy_b(b):
        s, r = lax.rem(b, 4), lax.rem(b, 8)
        return remote(sb.at[s], rb.at[r], send_b.at[s], recv_b.at[r], peer)

    def copy_c(b):
        r = lax.rem(b, 8)
        return remote(out.at[b, core, chip], out.at[b, core, chip], send_c.at[r], recv_c.at[r], peer)

    def copy_e(b):
        r = lax.rem(b, 8)
        return remote(out.at[b, core, chip], out.at[b, core, chip], send_e.at[r], recv_e.at[r], sibling)

    def copy_d(b):
        r = lax.rem(b, 8)
        return remote(out.at[b, core, 1 - chip], out.at[b, core, 1 - chip], send_d.at[r], recv_d.at[r], sibling)

    for n in range(ns):
        x_copy(n).start()
        if n % per == per - 1:
            w_copy(0, n // per).start()

    barrier = pltpu.get_barrier_semaphore()
    for other in (sibling, peer):
        pl.semaphore_signal(barrier, inc=1, device_id=other, device_id_type=MESH)
    pl.semaphore_wait(barrier, 2)

    row = lax.broadcasted_iota(jnp.int32, (TILE, XC), 0)

    def pack(n):
        stage = stages[n % ns]
        x_copy(n).wait()
        if n == nx - 1:
            for k in range(nk):
                w_copy(1, k).start()
        first = stage[table_ref[LONE_SOURCE]][0:1, :].astype(jnp.float32)
        lone[...] = jnp.broadcast_to(first, (TILE, XC)).astype(lone.dtype)

        def tile(t, carry):
            at = pl.ds(pl.multiple_of(t * TILE, TILE), TILE)
            xp[at, n * XC:(n + 1) * XC] = jnp.where(row + 1 == table_ref[MERGE + t], lone[...], stage[table_ref[t]])
            return carry

        lax.fori_loop(0, rows // TILE, tile, 0)
        if n + ns < nx:
            x_copy(n + ns).start()
            if (n + ns) % per == per - 1:
                w_copy(0, (n + ns) // per).start()

    def pack_for(k):
        for n in range(k * per, (k + 1) * per):
            pack(n)

    def reduce_on(i):
        @pl.when(jnp.logical_and(i >= 1, i - 1 < blocks))
        def _():
            b = i - 1
            s, q = lax.rem(b, 2), lax.rem(b, 4)
            copy_a(b).wait()
            there = pl.ds(pl.multiple_of((1 - chip) * half, 8), half)
            here = pl.ds(pl.multiple_of(chip * half, 8), half)
            sb[q] = part[s, core, there, :] + ra[s, there, :]
            so[q] = part[s, core, here, :] + ra[s, here, :]
            copy_b(b).start()

    def finish(i):
        @pl.when(jnp.logical_and(i >= 2, i - 2 < blocks))
        def _():
            b = i - 2
            copy_b(b).wait()
            out[b, core, chip] = (so[lax.rem(b, 4)] + rb[lax.rem(b, 8)]).astype(out.dtype)
            copy_c(b).start()
            copy_e(b).start()

        @pl.when(jnp.logical_and(i >= 4, i - 4 < blocks))
        def _():
            copy_c(i - 4).wait()
            copy_d(i - 4).start()

        @pl.when(jnp.logical_and(i >= 5, i - 5 < blocks))
        def _():
            copy_e(i - 5).wait()
            copy_d(i - 5).wait()

    def step(j, carry):
        i, k = j // nk, lax.rem(j, nk)
        for early in range(nk):
            pl.when(j == early)(functools.partial(pack_for, early))

        @pl.when(k == jnp.where(i <= 3, 1, 2))
        def _():
            reduce_on(i)

        @pl.when(k == nk - 1)
        def _():
            finish(i)

        @pl.when(i < blocks)
        def _():
            @pl.when(jnp.logical_and(i >= 1, i + 1 < blocks))
            def _():
                w_copy(i + 1, k).start()

            w_copy(i, k).wait()
            s = lax.rem(i, 2)
            deep = pl.ds(pl.multiple_of(k * KC, KC), KC)
            split = rows // (2 * TILE) * TILE
            for part_rows in (slice(0, split), slice(split, rows)):
                prod = jnp.dot(xp[part_rows, deep], wbuf[s, deep, :], preferred_element_type=jnp.float32)
                for h in range(2):
                    part[s, h, part_rows] = jnp.where(k == 0, 0.0, part[s, h, part_rows]) + prod[:, h * HB:(h + 1) * HB]

            @pl.when(k == nk - 1)
            def _():
                copy_a(i).start()

        return carry

    lax.fori_loop(0, nk * (blocks + LAST), step, 0)


def unpack_kernel(lens_ref, table_ref, packed, y_ref, spread, osem):
    slots = lens_ref.shape[0]
    chunks, tokens, width = spread.shape
    slot_tiles = tokens // slots // TILE
    row = lax.broadcasted_iota(jnp.int32, (TILE, HB), 0)

    def store(c):
        return pltpu.make_async_copy(spread.at[c], y_ref.at[:, pl.ds(pl.multiple_of(c * width, width), width)], osem.at[c])

    def chunk(c, carry):
        def move(source, target, count, length=None):
            source = pl.multiple_of(source * TILE, TILE)
            target = pl.multiple_of(target * TILE, TILE)
            for j in range(width // HB):
                piece = packed[c * PER + j // 2, j % 2, pl.ds(source, count * TILE), :]
                if length is not None:
                    piece = jnp.where(row < length, piece, jnp.zeros_like(piece))
                spread[c, pl.ds(target, count * TILE), j * HB:(j + 1) * HB] = piece

        def clear(target, count):
            at = pl.ds(pl.multiple_of(target * TILE, TILE), count * TILE)
            spread[c, at, :] = jnp.zeros((count * TILE, width), spread.dtype)

        @pl.loop(0, slots)
        def _(s):
            merged = jnp.logical_and(table_ref[LONE_TILE] > 0, table_ref[LONE_SLOT] == s)
            length = jnp.where(merged, 0, lens_ref[s])
            full = lax.div(length, TILE)
            used = lax.div(length + TILE - 1, TILE)
            source, target = table_ref[OFFS + s], s * slot_tiles
            quads = lax.div(full, 4)
            empty = lax.div(used + 3, 4)

            @pl.loop(0, quads)
            def _(t):
                move(source + 4 * t, target + 4 * t, 4)

            @pl.loop(quads * 4, full)
            def _(t):
                move(source + t, target + t, 1)

            @pl.when(full < used)
            def _():
                move(source + full, target + full, 1, length - full * TILE)

            @pl.loop(used, empty * 4)
            def _(t):
                clear(target + t, 1)

            @pl.loop(empty, slot_tiles // 4)
            def _(t):
                clear(target + 4 * t, 4)

        @pl.when(table_ref[LONE_TILE] > 0)
        def _():
            source = pl.multiple_of((table_ref[LONE_TILE] - 1) * TILE, TILE)
            target = pl.multiple_of(table_ref[LONE_SLOT] * (slot_tiles * TILE), TILE)
            for j in range(width // HB):
                piece = packed[c * PER + j // 2, j % 2, pl.ds(source, TILE), :].astype(jnp.float32)
                line = jnp.sum(jnp.where(row == table_ref[LONE_ROW], piece, 0.0), axis=0, keepdims=True)
                spread[c, pl.ds(target, TILE), j * HB:(j + 1) * HB] = jnp.where(row == 0, line, 0.0).astype(spread.dtype)

        store(c).start()
        return carry

    lax.fori_loop(0, chunks, chunk, 0)
    for c in range(chunks):
        store(c).wait()


def branch(index, rows, x_loc, w_loc, lengths, table):
    tokens, depth = x_loc.shape
    cols = w_loc.shape[1]
    blocks = cols // NB
    half = rows // 2
    f32, bf16 = jnp.float32, x_loc.dtype
    dma = pltpu.SemaphoreType.DMA
    buffers = 4 if rows <= 704 else 3 if rows <= 736 else 2
    grant = 2 * (rows * depth + buffers * tokens * XC + TILE * XC + 2 * depth * NB) + 4 * 14 * rows * HB + 500_000
    packed = pl.pallas_call(
        functools.partial(fused_kernel, rows),
        out_shape=pltpu.VMEM((blocks, 2, 2, half, HB), bf16),
        in_specs=[pl.BlockSpec(memory_space=pltpu.SMEM), pl.BlockSpec(memory_space=pl.ANY), pl.BlockSpec(memory_space=pl.ANY)],
        out_specs=pl.BlockSpec(memory_space=pltpu.VMEM),
        scratch_shapes=[
            pltpu.VMEM((rows, depth), bf16),
            pltpu.VMEM((TILE, XC), bf16),
            pltpu.VMEM((2, depth, NB), bf16),
            pltpu.VMEM((2, 2, rows, HB), f32),
            pltpu.VMEM((2, rows, HB), f32),
            pltpu.VMEM((4, half, HB), f32),
            pltpu.VMEM((4, half, HB), f32),
            pltpu.VMEM((8, half, HB), f32),
            dma((buffers,)), dma((2, depth // KC)), dma((2,)), dma((2,)), dma((4,)), dma((8,)),
            dma((8,)), dma((8,)), dma((8,)), dma((8,)), dma((8,)), dma((8,)),
            *[pltpu.VMEM((tokens // TILE, TILE, XC), bf16)] * buffers,
        ],
        compiler_params=pltpu.CompilerParams(collective_id=index, has_side_effects=True, vmem_limit_bytes=grant),
        cost_estimate=pl.CostEstimate(flops=2 * rows * depth * cols, bytes_accessed=2 * depth * cols, transcendentals=0),
        name=f"fused_{rows}",
    )(table, x_loc.reshape(tokens // TILE, TILE, depth), w_loc)
    packed = packed.reshape(blocks, 2, rows, HB)
    chunks = blocks // PER
    return pl.pallas_call(
        unpack_kernel,
        out_shape=jax.ShapeDtypeStruct((tokens, cols), bf16),
        in_specs=[pl.BlockSpec(memory_space=pltpu.SMEM), pl.BlockSpec(memory_space=pltpu.SMEM), pl.BlockSpec(memory_space=pltpu.VMEM)],
        out_specs=pl.BlockSpec(memory_space=pl.ANY),
        scratch_shapes=[
            pltpu.VMEM((chunks, tokens, PER * NB), bf16),
            dma((chunks,)),
        ],
        compiler_params=pltpu.CompilerParams(vmem_limit_bytes=27_000_000),
        cost_estimate=pl.CostEstimate(flops=0, bytes_accessed=2 * (rows + tokens) * cols, transcendentals=0),
        name=f"unpack_{rows}",
    )(lengths, table, packed)


def table_kernel(tokens, lens_ref, table_ref, index_ref):
    slots = lens_ref.shape[0]
    slot_tiles = tokens // slots // TILE
    lens = [lens_ref[s] for s in range(slots)]
    lone = jnp.int32(slots - 1)
    for s in reversed(range(slots - 1)):
        lone = jnp.where(lens[s] == 1, s, lone)
    rest = [lax.rem(lens[s], TILE) for s in range(slots)]
    host = jnp.int32(-1)
    for s in reversed(range(slots)):
        host = jnp.where(jnp.logical_and(lone != s, rest[s] != 0), s, host)
    offs, total = [], jnp.int32(0)
    lone_tile, lone_row = jnp.int32(0), jnp.int32(0)
    for s in range(slots):
        offs.append(total)
        tiles = jnp.where(jnp.logical_and(host >= 0, lone == s), 0, lax.div(lens[s] + (TILE - 1), TILE))
        total = total + tiles
        lone_tile = jnp.where(host == s, total, lone_tile)
        lone_row = jnp.where(host == s, rest[s], lone_row)

    def tile(t, carry):
        source = t
        for s in range(1, slots):
            source = jnp.where(t >= offs[s], s * slot_tiles + t - offs[s], source)
        table_ref[t] = jnp.where(t < total, source, 0)
        table_ref[MERGE + t] = jnp.where(t + 1 == lone_tile, lone_row + 1, 0)
        return carry

    lax.fori_loop(0, OFFS, tile, 0)
    for s in range(slots):
        table_ref[OFFS + s] = offs[s]
    table_ref[LONE_TILE] = lone_tile
    table_ref[LONE_ROW] = lone_row
    table_ref[LONE_SLOT] = lone
    table_ref[LONE_SOURCE] = lone * slot_tiles
    index = jnp.int32(0)
    for size in BUCKETS[:-1]:
        index = index + (total * TILE > size).astype(jnp.int32)
    index_ref[0] = index


def make_table(lengths, tokens):
    smem = pl.BlockSpec(memory_space=pltpu.SMEM)
    return pl.pallas_call(
        functools.partial(table_kernel, tokens),
        out_shape=(jax.ShapeDtypeStruct((128,), jnp.int32), jax.ShapeDtypeStruct((1,), jnp.int32)),
        in_specs=[smem],
        out_specs=(smem, smem),
        name="table",
    )(lengths)


def solution(mesh):
    def local_part(x_loc, w_loc, lengths):
        table, index = make_table(lengths, x_loc.shape[0])
        return lax.switch(index[0], [functools.partial(branch, j, rows) for j, rows in enumerate(BUCKETS)], x_loc, w_loc, lengths, table)

    return jax.shard_map(local_part, mesh=mesh, in_specs=(P("data", "tp"), P("tp", None), P("data")), out_specs=P("data", None), check_vma=False)
```

```python
import functools

import jax
import jax.numpy as jnp
from jax import lax
from jax.experimental import pallas as pl
from jax.experimental.pallas import tpu as pltpu
from jax.sharding import PartitionSpec as P

MESH = pl.DeviceIdType.MESH
TILE = 16
NB = 256
HB = NB // 2
XC = 1536
BUCKETS = (352, 416, 448) + tuple(range(480, 753, 16)) + (784,)
PER = 4
LAST = 5
OFFS, LONE_TILE, LONE_ROW, LONE_SLOT, LONE_SOURCE, MERGE = 50, 54, 55, 56, 57, 64


def chunk_depth(rows):
    return 6144 if rows <= 480 else 3072


def fused_kernel(rows, table_ref, x_ref, w_ref, out, *scratch):
    (xp, lone, wbuf, part, ra, sb, so, rb, xsem, wsem, send_a, recv_a, send_b, recv_b, send_c, recv_c, send_e, recv_e,
     send_d, recv_d, *stages) = scratch
    depth, cols = w_ref.shape
    blocks = cols // NB
    half = rows // 2
    ns = len(stages)
    me = lax.axis_index("tp")
    core = lax.rem(me, 2)
    chip = me // 2
    sibling = {"tp": me + 1 - 2 * core}
    peer = {"tp": lax.rem(me + 2, 4)}
    kc = chunk_depth(rows)
    nk = depth // kc
    nx = depth // XC
    per = nx // nk

    def x_copy(n):
        return pltpu.make_async_copy(x_ref.at[:, :, pl.ds(n * XC, XC)], stages[n % ns], xsem.at[n % ns])

    def w_copy(b, k):
        s = lax.rem(b, 2)
        deep = pl.ds(pl.multiple_of(k * kc, kc), kc)
        return pltpu.make_async_copy(w_ref.at[deep, pl.ds(pl.multiple_of(b * NB, NB), NB)], wbuf.at[s, deep], wsem.at[s, k])

    def remote(src, dst, ssem, rsem, to):
        return pltpu.make_async_remote_copy(src_ref=src, dst_ref=dst, send_sem=ssem, recv_sem=rsem, device_id=to, device_id_type=MESH)

    def copy_a(b):
        s = lax.rem(b, 2)
        return remote(part.at[s, 1 - core], ra.at[s], send_a.at[s], recv_a.at[s], sibling)

    def copy_b(b):
        s, r = lax.rem(b, 4), lax.rem(b, 8)
        return remote(sb.at[s], rb.at[r], send_b.at[s], recv_b.at[r], peer)

    def copy_c(b):
        r = lax.rem(b, 8)
        return remote(out.at[b, core, chip], out.at[b, core, chip], send_c.at[r], recv_c.at[r], peer)

    def copy_e(b):
        r = lax.rem(b, 8)
        return remote(out.at[b, core, chip], out.at[b, core, chip], send_e.at[r], recv_e.at[r], sibling)

    def copy_d(b):
        r = lax.rem(b, 8)
        return remote(out.at[b, core, 1 - chip], out.at[b, core, 1 - chip], send_d.at[r], recv_d.at[r], sibling)

    for n in range(ns):
        x_copy(n).start()
        if n % per == per - 1:
            w_copy(0, n // per).start()

    barrier = pltpu.get_barrier_semaphore()
    for other in (sibling, peer):
        pl.semaphore_signal(barrier, inc=1, device_id=other, device_id_type=MESH)
    pl.semaphore_wait(barrier, 2)

    row = lax.broadcasted_iota(jnp.int32, (TILE, XC), 0)

    def pack(n):
        stage = stages[n % ns]
        x_copy(n).wait()
        if n == nx - 1:
            for k in range(nk):
                w_copy(1, k).start()
        first = stage[table_ref[LONE_SOURCE]][0:1, :].astype(jnp.float32)
        lone[...] = jnp.broadcast_to(first, (TILE, XC)).astype(lone.dtype)

        def tile(t, carry):
            at = pl.ds(pl.multiple_of(t * TILE, TILE), TILE)
            xp[at, n * XC:(n + 1) * XC] = jnp.where(row + 1 == table_ref[MERGE + t], lone[...], stage[table_ref[t]])
            return carry

        lax.fori_loop(0, rows // TILE, tile, 0)
        if n + ns < nx:
            x_copy(n + ns).start()
            if (n + ns) % per == per - 1:
                w_copy(0, (n + ns) // per).start()

    def pack_for(k):
        for n in range(k * per, (k + 1) * per):
            pack(n)

    def reduce_on(i):
        @pl.when(jnp.logical_and(i >= 1, i - 1 < blocks))
        def _():
            b = i - 1
            s, q = lax.rem(b, 2), lax.rem(b, 4)
            copy_a(b).wait()
            there = pl.ds(pl.multiple_of((1 - chip) * half, 8), half)
            here = pl.ds(pl.multiple_of(chip * half, 8), half)
            sb[q] = part[s, core, there, :] + ra[s, there, :]
            so[q] = part[s, core, here, :] + ra[s, here, :]
            copy_b(b).start()

    def finish(i):
        @pl.when(jnp.logical_and(i >= 2, i - 2 < blocks))
        def _():
            b = i - 2
            copy_b(b).wait()
            out[b, core, chip] = (so[lax.rem(b, 4)] + rb[lax.rem(b, 8)]).astype(out.dtype)
            copy_c(b).start()
            copy_e(b).start()

        @pl.when(jnp.logical_and(i >= 4, i - 4 < blocks))
        def _():
            copy_c(i - 4).wait()
            copy_d(i - 4).start()

        @pl.when(jnp.logical_and(i >= 5, i - 5 < blocks))
        def _():
            copy_e(i - 5).wait()
            copy_d(i - 5).wait()

    def step(j, carry):
        i, k = j // nk, lax.rem(j, nk)
        for early in range(nk):
            pl.when(j == early)(functools.partial(pack_for, early))

        @pl.when(k == jnp.where(i <= 3, 1, min(2, nk - 1)))
        def _():
            reduce_on(i)

        @pl.when(k == nk - 1)
        def _():
            finish(i)

        @pl.when(i < blocks)
        def _():
            @pl.when(jnp.logical_and(i >= 1, i + 1 < blocks))
            def _():
                w_copy(i + 1, k).start()

            w_copy(i, k).wait()
            s = lax.rem(i, 2)
            deep = pl.ds(pl.multiple_of(k * kc, kc), kc)
            split = rows // (2 * TILE) * TILE
            for part_rows in (slice(0, split), slice(split, rows)):
                prod = jnp.dot(xp[part_rows, deep], wbuf[s, deep, :], preferred_element_type=jnp.float32)
                for h in range(2):
                    part[s, h, part_rows] = jnp.where(k == 0, 0.0, part[s, h, part_rows]) + prod[:, h * HB:(h + 1) * HB]

            @pl.when(k == nk - 1)
            def _():
                copy_a(i).start()

        return carry

    lax.fori_loop(0, nk * (blocks + LAST), step, 0)


def unpack_kernel(lens_ref, table_ref, packed, y_ref, spread, osem):
    slots = lens_ref.shape[0]
    chunks, tokens, width = spread.shape
    slot_tiles = tokens // slots // TILE
    row = lax.broadcasted_iota(jnp.int32, (TILE, HB), 0)

    def store(c):
        return pltpu.make_async_copy(spread.at[c], y_ref.at[:, pl.ds(pl.multiple_of(c * width, width), width)], osem.at[c])

    def chunk(c, carry):
        def move(source, target, count, length=None):
            source = pl.multiple_of(source * TILE, TILE)
            target = pl.multiple_of(target * TILE, TILE)
            for j in range(width // HB):
                piece = packed[c * PER + j // 2, j % 2, pl.ds(source, count * TILE), :]
                if length is not None:
                    piece = jnp.where(row < length, piece, jnp.zeros_like(piece))
                spread[c, pl.ds(target, count * TILE), j * HB:(j + 1) * HB] = piece

        def clear(target, count):
            at = pl.ds(pl.multiple_of(target * TILE, TILE), count * TILE)
            spread[c, at, :] = jnp.zeros((count * TILE, width), spread.dtype)

        @pl.loop(0, slots)
        def _(s):
            merged = jnp.logical_and(table_ref[LONE_TILE] > 0, table_ref[LONE_SLOT] == s)
            length = jnp.where(merged, 0, lens_ref[s])
            full = lax.div(length, TILE)
            used = lax.div(length + TILE - 1, TILE)
            source, target = table_ref[OFFS + s], s * slot_tiles
            quads = lax.div(full, 4)
            empty = lax.div(used + 3, 4)

            @pl.loop(0, quads)
            def _(t):
                move(source + 4 * t, target + 4 * t, 4)

            @pl.loop(quads * 4, full)
            def _(t):
                move(source + t, target + t, 1)

            @pl.when(full < used)
            def _():
                move(source + full, target + full, 1, length - full * TILE)

            @pl.loop(used, empty * 4)
            def _(t):
                clear(target + t, 1)

            @pl.loop(empty, slot_tiles // 4)
            def _(t):
                clear(target + 4 * t, 4)

        @pl.when(table_ref[LONE_TILE] > 0)
        def _():
            source = pl.multiple_of((table_ref[LONE_TILE] - 1) * TILE, TILE)
            target = pl.multiple_of(table_ref[LONE_SLOT] * (slot_tiles * TILE), TILE)
            for j in range(width // HB):
                piece = packed[c * PER + j // 2, j % 2, pl.ds(source, TILE), :].astype(jnp.float32)
                line = jnp.sum(jnp.where(row == table_ref[LONE_ROW], piece, 0.0), axis=0, keepdims=True)
                spread[c, pl.ds(target, TILE), j * HB:(j + 1) * HB] = jnp.where(row == 0, line, 0.0).astype(spread.dtype)

        store(c).start()
        return carry

    lax.fori_loop(0, chunks, chunk, 0)
    for c in range(chunks):
        store(c).wait()


def branch(index, rows, x_loc, w_loc, lengths, table):
    tokens, depth = x_loc.shape
    cols = w_loc.shape[1]
    blocks = cols // NB
    half = rows // 2
    f32, bf16 = jnp.float32, x_loc.dtype
    dma = pltpu.SemaphoreType.DMA
    buffers = 4 if rows <= 704 else 3 if rows <= 736 else 2
    grant = 2 * (rows * depth + buffers * tokens * XC + TILE * XC + 2 * depth * NB) + 4 * 14 * rows * HB + 500_000
    packed = pl.pallas_call(
        functools.partial(fused_kernel, rows),
        out_shape=pltpu.VMEM((blocks, 2, 2, half, HB), bf16),
        in_specs=[pl.BlockSpec(memory_space=pltpu.SMEM), pl.BlockSpec(memory_space=pl.ANY), pl.BlockSpec(memory_space=pl.ANY)],
        out_specs=pl.BlockSpec(memory_space=pltpu.VMEM),
        scratch_shapes=[
            pltpu.VMEM((rows, depth), bf16),
            pltpu.VMEM((TILE, XC), bf16),
            pltpu.VMEM((2, depth, NB), bf16),
            pltpu.VMEM((2, 2, rows, HB), f32),
            pltpu.VMEM((2, rows, HB), f32),
            pltpu.VMEM((4, half, HB), f32),
            pltpu.VMEM((4, half, HB), f32),
            pltpu.VMEM((8, half, HB), f32),
            dma((buffers,)), dma((2, depth // chunk_depth(rows))), dma((2,)), dma((2,)), dma((4,)), dma((8,)),
            dma((8,)), dma((8,)), dma((8,)), dma((8,)), dma((8,)), dma((8,)),
            *[pltpu.VMEM((tokens // TILE, TILE, XC), bf16)] * buffers,
        ],
        compiler_params=pltpu.CompilerParams(collective_id=index, has_side_effects=True, vmem_limit_bytes=grant),
        cost_estimate=pl.CostEstimate(flops=2 * rows * depth * cols, bytes_accessed=2 * depth * cols, transcendentals=0),
        name=f"fused_{rows}",
    )(table, x_loc.reshape(tokens // TILE, TILE, depth), w_loc)
    packed = packed.reshape(blocks, 2, rows, HB)
    chunks = blocks // PER
    return pl.pallas_call(
        unpack_kernel,
        out_shape=jax.ShapeDtypeStruct((tokens, cols), bf16),
        in_specs=[pl.BlockSpec(memory_space=pltpu.SMEM), pl.BlockSpec(memory_space=pltpu.SMEM), pl.BlockSpec(memory_space=pltpu.VMEM)],
        out_specs=pl.BlockSpec(memory_space=pl.ANY),
        scratch_shapes=[
            pltpu.VMEM((chunks, tokens, PER * NB), bf16),
            dma((chunks,)),
        ],
        compiler_params=pltpu.CompilerParams(vmem_limit_bytes=27_000_000),
        cost_estimate=pl.CostEstimate(flops=0, bytes_accessed=2 * (rows + tokens) * cols, transcendentals=0),
        name=f"unpack_{rows}",
    )(lengths, table, packed)


def table_kernel(tokens, lens_ref, table_ref, index_ref):
    slots = lens_ref.shape[0]
    slot_tiles = tokens // slots // TILE
    lens = [lens_ref[s] for s in range(slots)]
    lone = jnp.int32(slots - 1)
    for s in reversed(range(slots - 1)):
        lone = jnp.where(lens[s] == 1, s, lone)
    rest = [lax.rem(lens[s], TILE) for s in range(slots)]
    host = jnp.int32(-1)
    for s in reversed(range(slots)):
        host = jnp.where(jnp.logical_and(lone != s, rest[s] != 0), s, host)
    offs, total = [], jnp.int32(0)
    lone_tile, lone_row = jnp.int32(0), jnp.int32(0)
    for s in range(slots):
        offs.append(total)
        tiles = jnp.where(jnp.logical_and(host >= 0, lone == s), 0, lax.div(lens[s] + (TILE - 1), TILE))
        total = total + tiles
        lone_tile = jnp.where(host == s, total, lone_tile)
        lone_row = jnp.where(host == s, rest[s], lone_row)

    def tile(t, carry):
        source = t
        for s in range(1, slots):
            source = jnp.where(t >= offs[s], s * slot_tiles + t - offs[s], source)
        table_ref[t] = jnp.where(t < total, source, 0)
        table_ref[MERGE + t] = jnp.where(t + 1 == lone_tile, lone_row + 1, 0)
        return carry

    lax.fori_loop(0, OFFS, tile, 0)
    for s in range(slots):
        table_ref[OFFS + s] = offs[s]
    table_ref[LONE_TILE] = lone_tile
    table_ref[LONE_ROW] = lone_row
    table_ref[LONE_SLOT] = lone
    table_ref[LONE_SOURCE] = lone * slot_tiles
    index = jnp.int32(0)
    for size in BUCKETS[:-1]:
        index = index + (total * TILE > size).astype(jnp.int32)
    index_ref[0] = index


def make_table(lengths, tokens):
    smem = pl.BlockSpec(memory_space=pltpu.SMEM)
    return pl.pallas_call(
        functools.partial(table_kernel, tokens),
        out_shape=(jax.ShapeDtypeStruct((128,), jnp.int32), jax.ShapeDtypeStruct((1,), jnp.int32)),
        in_specs=[smem],
        out_specs=(smem, smem),
        name="table",
    )(lengths)


def solution(mesh):
    def local_part(x_loc, w_loc, lengths):
        table, index = make_table(lengths, x_loc.shape[0])
        return lax.switch(index[0], [functools.partial(branch, j, rows) for j, rows in enumerate(BUCKETS)], x_loc, w_loc, lengths, table)

    return jax.shard_map(local_part, mesh=mesh, in_specs=(P("data", "tp"), P("tp", None), P("data")), out_specs=P("data", None), check_vma=False)
```
